128 devices in a mesh: layer: 2 (over core), px: 16 (over x, z), py: 4 (over y).
Axes of the slice: x: 4, y: 4, z: 4, core: 2. Of those that a mesh axis runs over, the one named last changes fastest.
Arguments:
- right_side: float32 [8, 2048, 4096], P('layer', 'px', 'py'), may hold values from -30 to 30
- row_conduct: float32 [8, 2048, 4096], P('layer', 'px', 'py'), may hold values from 0.5 to 2
- column_conduct: float32 [8, 2048, 4096], P('layer', 'px', 'py'), may hold values from 0.5 to 2
- via_conduct: float32 [8, 2048, 4096], P('layer', 'px', 'py'), may hold values from 0.5 to 4
- via_mask: int32 [8, 2048, 4096], P('layer', 'px', 'py'), may hold values 0 or 1
- ground_conduct: float32 [8, 2048, 4096], P('layer', 'px', 'py'), may hold values from 0.01 to 0.1
Outputs:
- solution_field: float32 [8, 2048, 4096], P('layer', 'px', 'py')
- residual: float32 [8, 2048, 4096], P('layer', 'px', 'py')
The draws below stay inside these ranges and needn't reach their ends.
All inputs are finite; a program needn't handle non-finite values. No bound on the sum of `via_mask` on one device may be relied on, other than what follows from the above.
Results may differ from the reference program's by a relative error of at most 0.0001.
Values sent between devices are 32-bit elements; how exact they have to be, the bound alone decides.
A program may use at most 128 MiB of HBM per device.

```python
import math
import jax
import jax.numpy as jnp

ITERS = 2
LAYERS = 8
NX = 2048
NY = 4096


def draw_right_side(key, part):
    noise = jax.random.normal(key, (LAYERS, NX, NY), jnp.float32)
    rows = jnp.arange(NX, dtype=jnp.float32) / NX
    ramp = jnp.exp(jnp.log(3.0) * rows)[None, :, None]
    value = noise * ramp
    return jnp.clip(value, -30.0, 30.0)


def touch_ends(drawn, own_key, smallest, high):
    spot = [jax.random.randint(jax.random.fold_in(own_key, axis), (), 0, length) for axis, length in enumerate(drawn.shape)]
    longest = drawn.shape.index(max(drawn.shape))
    next_to = spot[:longest] + [(spot[longest] + 1) % drawn.shape[longest]] + spot[longest + 1:]
    return drawn.at[tuple(spot)].set(smallest).at[tuple(next_to)].set(high)


def shard_levels(key, dims, cuts, low, top_value):
    loudness = 1.0
    for dim, parts in cuts:
        heights = jax.random.uniform(jax.random.fold_in(jax.random.fold_in(key, 6), dim), (parts,), jnp.float32, low / len(cuts), top_value / len(cuts))
        loudness = loudness * jnp.repeat(jnp.exp(heights), dims[dim] // parts).reshape((-1,) + (1,) * (len(dims) - 1 - dim))
    return loudness


def setup_inputs(seed: int = 0) -> dict:
    streams_of = jax.random.split(jax.random.key(seed), 7)
    return {
        "right_side": draw_right_side(jax.random.fold_in(streams_of[6], 71), 0),
        "row_conduct": jnp.clip(jnp.exp(math.log(2.0) - 1.3862944 * jax.random.uniform(streams_of[1], (LAYERS, NX, NY), jnp.float32) ** shard_levels(streams_of[1], (LAYERS, NX, NY), ((0, 2), (1, 16), (2, 4)), -0.2, 0.2)), 0.5, 2.0),
        "column_conduct": jnp.clip(jnp.exp(math.log(2.0) - 1.3862944 * jax.random.uniform(streams_of[2], (LAYERS, NX, NY), jnp.float32) ** shard_levels(streams_of[2], (LAYERS, NX, NY), ((0, 2), (1, 16), (2, 4)), -0.2, 0.2)), 0.5, 2.0),
        "via_conduct": jnp.clip(jnp.exp(math.log(4.0) - 2.0794415 * jax.random.uniform(streams_of[3], (LAYERS, NX, NY), jnp.float32) ** shard_levels(streams_of[3], (LAYERS, NX, NY), ((0, 2), (1, 16), (2, 4)), -0.2, 0.2)), 0.5, 4.0),
        "via_mask": touch_ends((jax.random.randint(streams_of[4], (LAYERS, NX, NY), 0, 4) < 3).astype(jnp.int32), jax.random.fold_in(streams_of[4], 1), 0, 1),
        "ground_conduct": jnp.clip(jnp.exp(math.log(0.1) - 2.3025851 * jax.random.uniform(streams_of[5], (LAYERS, NX, NY), jnp.float32) ** shard_levels(streams_of[5], (LAYERS, NX, NY), ((0, 2), (1, 16), (2, 4)), -0.2, 0.2)), 0.01, 0.1),
    }


def factor_layers(diagonal, vertical, vertical_below, carried):
    gains = []
    inverses = []
    previous = carried
    for index in range(diagonal.shape[0]):
        inverse = 1.0 / (diagonal[index] - vertical_below[index] * previous)
        previous = vertical[index] * inverse
        gains.append(previous)
        inverses.append(inverse)
    return jnp.stack(gains), jnp.stack(inverses)


def forward_layers(residual, vertical_below, inverses, carried):
    values = []
    previous = carried
    for index in range(residual.shape[0]):
        previous = (residual[index] + vertical_below[index] * previous) * inverses[index]
        values.append(previous)
    return jnp.stack(values)


def back_layers(forward, gains, carried):
    count = forward.shape[0]
    values = [None] * count
    following = carried
    for index in range(count - 1, -1, -1):
        following = forward[index] + gains[index] * following
        values[index] = following
    return jnp.stack(values)


def operate(field, coeffs):
    diagonal, row_conduct, row_upper, column_conduct, column_left, vertical, vertical_below = coeffs
    padded = jnp.pad(field, 1)
    return (diagonal * field
            - row_conduct * padded[1:-1, 2:, 1:-1]
            - row_upper * padded[1:-1, :-2, 1:-1]
            - column_conduct * padded[1:-1, 1:-1, 2:]
            - column_left * padded[1:-1, 1:-1, :-2]
            - vertical * padded[2:, 1:-1, 1:-1]
            - vertical_below * padded[:-2, 1:-1, 1:-1])


def reference(right_side, row_conduct, column_conduct, via_conduct, via_mask, ground_conduct):
    level = jnp.arange(LAYERS, dtype=jnp.int32)
    keep = (level < LAYERS - 1).astype(right_side.dtype)[:, None, None]
    vertical = via_conduct * via_mask.astype(right_side.dtype) * keep
    row_upper = jnp.concatenate([jnp.zeros_like(row_conduct[:, :1, :]), row_conduct[:, :-1, :]], axis=1)
    column_left = jnp.concatenate([jnp.zeros_like(column_conduct[:, :, :1]), column_conduct[:, :, :-1]], axis=2)
    vertical_below = jnp.concatenate([jnp.zeros_like(vertical[:1]), vertical[:-1]], axis=0)
    diagonal = ground_conduct + row_conduct + row_upper + column_conduct + column_left + vertical + vertical_below
    coeffs = (diagonal, row_conduct, row_upper, column_conduct, column_left, vertical, vertical_below)
    plane = jnp.zeros_like(right_side[0])
    gains, inverses = factor_layers(diagonal, vertical, vertical_below, plane)

    def precondition(residual):
        forward = forward_layers(residual, vertical_below, inverses, plane)
        return back_layers(forward, gains, plane)

    solution_field = jnp.zeros_like(right_side)
    residual = right_side
    precond = precondition(residual)
    direction = precond
    rho = jnp.sum(residual * precond)
    for step in range(ITERS):
        image = operate(direction, coeffs)
        alpha = rho / jnp.sum(direction * image)
        solution_field = solution_field + alpha * direction
        residual = residual - alpha * image
        if step + 1 < ITERS:
            precond = precondition(residual)
            rho_next = jnp.sum(residual * precond)
            direction = precond + (rho_next / rho) * direction
            rho = rho_next
    return solution_field, residual
```

```python
import functools

import jax
import jax.numpy as jnp
from jax import lax
from jax.experimental import pallas as pl
from jax.experimental.pallas import tpu as pltpu
from jax.sharding import PartitionSpec as P

MESH = pl.DeviceIdType.MESH
S = 8
L = 128
F32 = jnp.float32


def kernel(sizes, chunks, b_hbm, r_hbm, c_hbm, via_hbm, mask_hbm, g_hbm, bb, zb, vb, wb, ut, coef,
           rb, cb, ub, mb, gb, vm, vmask, gain, inv, mid, ef, efo, f2, f2o,
           redge, cedge, pprev, colacc, row_s, row_r, col_s, col_r, red_s, red_r, sum_s, sum_r,
           load_sem, edge_sem, top_sem, vm_sem, ef_sem, f2_sem, halo_sem, red_sem, sum_sem):
    members, npx, npy = sizes
    depth, rows, width = bb.shape
    tiles = rows // S
    per = tiles // chunks
    last = depth - 1
    blocks = width // L
    up = lax.axis_index("layer")
    px = lax.axis_index("px")
    py = lax.axis_index("py")
    lower = up == 0
    lay = [k + up * (last - 2 * k) for k in range(depth)]
    via_at = [k + up * (last - 1 - 2 * k) for k in range(last)]
    chunk_rows = per * S
    peers = npx * npy
    me = px * npy + py

    partner = (1 - up, px, py)
    above, below = (up, px - 1, py), (up, px + 1, py)
    left, right = (up, px, py - 1), (up, px, py + 1)

    def peer(d):
        t = lax.rem(me + d, peers)
        return (up, t // npy, lax.rem(t, npy))

    row_r[...] = jnp.zeros_like(row_r)
    col_r[...] = jnp.zeros_like(col_r)
    barrier = pltpu.get_barrier_semaphore()
    pl.semaphore_signal(barrier, inc=1, device_id=partner, device_id_type=MESH)

    def greet(d, _):
        pl.semaphore_signal(barrier, inc=1, device_id=peer(d), device_id_type=MESH)
        return 0

    edge_loads = [
        pltpu.make_async_copy(r_hbm.at[:, pl.ds(rows - S, S)], redge, edge_sem.at[0]),
        pltpu.make_async_copy(c_hbm.at[:, :, pl.ds(width - L, L)], cedge, edge_sem.at[1]),
    ]
    for copy in edge_loads:
        copy.start()
    top = [
        pltpu.make_async_copy(via_hbm.at[last], vm, top_sem.at[0]),
        pltpu.make_async_copy(mask_hbm.at[last], vmask, top_sem.at[1]),
    ]

    @pl.when(lower)
    def _():
        for copy in top:
            copy.start()

    def loads(c):
        start = pl.multiple_of(c * chunk_rows, chunk_rows)
        at = pl.ds(start, chunk_rows)
        pad = pl.ds(pl.multiple_of(start + S, S), chunk_rows)
        inner = pl.ds(0, last)
        pairs = [(via_hbm.at[inner, at], ub.at[:, at]), (mask_hbm.at[inner, at], mb.at[:, at]),
                 (r_hbm.at[:, at], rb.at[:, pad]), (c_hbm.at[:, at], cb.at[:, at]),
                 (g_hbm.at[:, at], gb.at[:, at]), (b_hbm.at[:, at], bb.at[:, at])]
        return [pltpu.make_async_copy(src, dst, load_sem.at[a, c]) for a, (src, dst) in enumerate(pairs)]

    for c in range(chunks):
        for copy in loads(c):
            copy.start()

    lax.fori_loop(1, peers, greet, 0)

    lane = lax.broadcasted_iota(jnp.int32, (S, L), 1)
    sub = lax.broadcasted_iota(jnp.int32, (S, L), 0)
    first_lane, final_lane = lane == 0, lane == L - 1
    first_sub, final_sub = sub == 0, sub == S - 1

    def remote(src, dst, sems, device):
        return pltpu.make_async_remote_copy(
            src_ref=src, dst_ref=dst, send_sem=sems.at[0], recv_sem=sems.at[1],
            device_id=device, device_id_type=MESH)

    def exchanges(trip):
        return (
            (px < npx - 1, px > 0, remote(row_s.at[trip, 0], row_r.at[trip, 0], halo_sem.at[trip, 0], below)),
            (px > 0, px < npx - 1, remote(row_s.at[trip, 1], row_r.at[trip, 1], halo_sem.at[trip, 1], above)),
            (py < npy - 1, py > 0, remote(col_s.at[trip, 0], col_r.at[trip, 0], halo_sem.at[trip, 2], right)),
            (py > 0, py < npy - 1, remote(col_s.at[trip, 1], col_r.at[trip, 1], halo_sem.at[trip, 3], left)),
        )

    def send_halo(trip, which):
        for e in which:
            sends, _, copy = exchanges(trip)[e]
            pl.when(sends)(copy.start)

    def take_halo(trip, which):
        for e in which:
            sends, takes, copy = exchanges(trip)[e]
            pl.when(takes)(copy.wait_recv)

    def end_halo(trip, which):
        for e in which:
            sends, _, copy = exchanges(trip)[e]
            pl.when(sends)(copy.wait_send)

    for copy in edge_loads:
        copy.wait()
    for k in range(depth):
        row_s[0, 0, k:k + 1, :] = redge[lay[k], S - 1:S, :]
        acc = jnp.zeros((S, L), F32)
        for i in range(tiles):
            edge = jnp.broadcast_to(cedge[lay[k], i * S:(i + 1) * S, L - 1:L], (S, L))
            acc = jnp.where(lane == sub + i * S, edge, acc)
        col_s[0, 0, k:k + 1, :] = jnp.sum(acc, axis=0, keepdims=True)

    vm_copy = remote(vm, vm, vm_sem, partner)

    @pl.when(lower)
    def _():
        for copy in top:
            copy.wait()

        def times(i, _):
            at = pl.ds(pl.multiple_of(i * S, S), S)
            vm[at, :] = vm[at, :] * vmask[at, :].astype(F32)
            return 0

        lax.fori_loop(0, tiles, times, 0)

    pl.semaphore_wait(barrier, peers)
    send_halo(0, (0, 2))
    pl.when(lower)(vm_copy.start)

    take_halo(0, (0, 2))
    for k in range(depth):
        rb[lay[k], S - 1:S, :] = row_r[0, 0, k:k + 1, :]

    def column(ref, k, i):
        spread = jnp.broadcast_to(ref[k:k + 1, :], (S, L))
        return jnp.sum(jnp.where(lane == sub + i * S, spread, 0.0), axis=1, keepdims=True)

    def rows_at(i):
        return pl.ds(pl.multiple_of(i * S, S), S)

    def cut(j):
        return pl.ds(j * L, L)

    def next_row(now, after):
        return pltpu.roll(jnp.where(first_sub, after, now), S - 1, 0)

    def prev_row(now, before):
        return pltpu.roll(jnp.where(final_sub, before, now), 1, 0)

    def from_left(parts, edge):
        turned = [pltpu.roll(p, 1, 1) for p in parts]
        return [jnp.where(first_lane, turned[j - 1] if j else edge, turned[j]) for j in range(blocks)]

    def from_right(parts, edge):
        turned = [pltpu.roll(p, L - 1, 1) for p in parts]
        return [jnp.where(final_lane, turned[j + 1] if j < blocks - 1 else edge, turned[j]) for j in range(blocks)]

    def factor_tile(i):
        at, pad = rows_at(i), rows_at(i + 1)
        coupling, g, y = [None] * blocks, [None] * blocks, [None] * blocks
        for k in range(depth):
            edge = column(col_r.at[0, 0], k, i)
            c = [cb[lay[k], at, cut(j)] for j in range(blocks)]
            c_left = from_left(c, edge)
            for j in range(blocks):
                r = rb[lay[k], pad, cut(j)]
                d = gb[lay[k], at, cut(j)] + r + prev_row(r, rb[lay[k], at, cut(j)]) + c[j] + c_left[j]
                rhs = bb[lay[k], at, cut(j)]
                if k:
                    d = d + coupling[j] - coupling[j] * g[j]
                    rhs = rhs + g[j] * y[j]
                y[j] = rhs
                if k < last:
                    coupling[j] = ub[via_at[k], at, cut(j)] * mb[via_at[k], at, cut(j)].astype(F32)
                    inverse = 1.0 / (d + coupling[j])
                    g[j] = coupling[j] * inverse
                    gain[k, at, cut(j)] = g[j]
                    inv[k, at, cut(j)] = inverse
                    zb[lay[k], pad, cut(j)] = rhs * inverse
                else:
                    ef[0, at, cut(j)] = d
                    ef[1, at, cut(j)] = rhs

    def chunk_at(c):
        return pl.ds(pl.multiple_of(c * chunk_rows, chunk_rows), chunk_rows)

    def ef_copy(c):
        return remote(ef.at[:, chunk_at(c)], efo.at[:, chunk_at(c)], ef_sem.at[c], partner)

    def f2_copy(c):
        return remote(f2.at[chunk_at(c)], f2o.at[chunk_at(c)], f2_sem.at[c], partner)

    def in_chunks(tile, before=None, after=None):
        def chunk(c, _):
            if before is not None:
                before(c)

            def one(j, _):
                tile(c * per + j)
                return 0

            lax.fori_loop(0, per, one, 0)
            if after is not None:
                after(c)
            return 0

        lax.fori_loop(0, chunks, chunk, 0)

    def wait_loads(c):
        for copy in loads(c):
            copy.wait()

    in_chunks(factor_tile, before=wait_loads, after=lambda c: ef_copy(c).start())

    @pl.when(up == 1)
    def _():
        vm_copy.wait_recv()

    def back(field, i, own):
        at, pad = rows_at(i), rows_at(i + 1)
        mine = lane == sub + i * S
        value = own
        for k in range(last, -1, -1):
            for j in range(blocks):
                if k < last:
                    value[j] = field[lay[k], pad, cut(j)] + gain[k, at, cut(j)] * value[j]
                field[lay[k], pad, cut(j)] = value[j]
            first = jnp.broadcast_to(value[0][:, 0:1], (S, L))
            final = jnp.broadcast_to(value[blocks - 1][:, L - 1:L], (S, L))
            colacc[0, k] = jnp.where(mine, final, colacc[0, k])
            colacc[1, k] = jnp.where(mine, first, colacc[1, k])

    def back_first(i):
        at = rows_at(i)
        value = []
        for j in range(blocks):
            e, f = ef[0, at, cut(j)], ef[1, at, cut(j)]
            eo, fo = efo[0, at, cut(j)], efo[1, at, cut(j)]
            v = vm[at, cut(j)]
            shared = 1.0 / (e * eo + v * (e + eo))
            own, cross = (eo + v) * shared, v * shared
            mid[0, at, cut(j)] = own
            mid[1, at, cut(j)] = cross
            value.append(own * f + cross * fo)
        back(zb, i, value)

    def back_second(i):
        at = rows_at(i)
        back(vb, i, [mid[0, at, cut(j)] * f2[at, cut(j)] + mid[1, at, cut(j)] * f2o[at, cut(j)] for j in range(blocks)])

    def exchange(field, trip):
        for k in range(depth):
            row_s[trip, 0, k:k + 1, :] = field[lay[k], rows + S - 1:rows + S, :]
            row_s[trip, 1, k:k + 1, :] = field[lay[k], S:S + 1, :]
            final = jnp.sum(colacc[0, k], axis=0, keepdims=True)
            col_s[trip, 0, k:k + 1, :] = final * col_s[0, 0, k:k + 1, :]
            col_s[trip, 1, k:k + 1, :] = jnp.sum(colacc[1, k], axis=0, keepdims=True)
        send_halo(trip, range(4))

    def receive(field, trip):
        take_halo(trip, range(4))
        for k in range(depth):
            field[lay[k], S - 1:S, :] = row_r[trip, 0, k:k + 1, :]
            field[lay[k], rows + S:rows + S + 1, :] = row_r[trip, 1, k:k + 1, :]
            for j in range(blocks):
                pprev[k, :, cut(j)] = rb[lay[k], 0:S, cut(j)] * field[lay[k], 0:S, cut(j)]

    def sideways(field, trip, i, k):
        at, pad, ahead = rows_at(i), rows_at(i + 1), rows_at(i + 2)
        value = [field[lay[k], pad, cut(j)] for j in range(blocks)]
        c = [cb[lay[k], at, cut(j)] for j in range(blocks)]
        before = column(col_r.at[trip, 0], k, i)
        after = column(col_r.at[trip, 1], k, i)
        to_right = from_left([c[j] * value[j] for j in range(blocks)], before)
        beside = from_right(value, after)
        out = []
        for j in range(blocks):
            r = rb[lay[k], pad, cut(j)]
            down = r * value[j]
            term = r * next_row(value[j], field[lay[k], ahead, cut(j)]) + prev_row(down, pprev[k, :, cut(j)])
            pprev[k, :, cut(j)] = down
            out.append(term + (c[j] * beside[j] + to_right[j]))
        return out, value

    def pack(one, two):
        one = jnp.sum(one, axis=0, keepdims=True)
        two = jnp.sum(two, axis=0, keepdims=True)
        one = one + pltpu.roll(one, L // 2, 1)
        two = two + pltpu.roll(two, L // 2, 1)
        return jnp.where(lane[0:1] < L // 2, one, two)

    def red_copy(slot):
        return remote(red_s.at[slot], red_r.at[slot], red_sem.at[slot], partner)

    def sum_begin(slot, one, two):
        red_s[slot] = pack(one, two)
        red_copy(slot).start()

    def sum_copy(slot, d):
        return remote(sum_s.at[slot], sum_r.at[slot, me], sum_sem.at[slot], peer(d))

    def sum_middle(slot):
        red_copy(slot).wait_recv()
        total = red_s[slot] + red_r[slot]
        sum_s[slot] = total
        sum_r[slot, me] = total

        def send(d, _):
            sum_copy(slot, d).start()
            return 0

        lax.fori_loop(1, peers, send, 0)

    def sum_bytes(slot, side):
        part = sum_r.at[slot, pl.ds(0, peers - 1)]
        return pltpu.make_async_copy(part, part, sum_sem.at[slot, side])

    def sum_finish(slot):
        sum_bytes(slot, 1).wait()
        total = jnp.sum(sum_r[slot], axis=0)
        low = jnp.sum(jnp.where(lane[0:1] < L // 2, total, 0.0), axis=1, keepdims=True)
        high = jnp.sum(jnp.where(lane[0:1] < L // 2, 0.0, total), axis=1, keepdims=True)
        return low, high

    def sum_end(slot):
        red_copy(slot).wait_send()
        sum_bytes(slot, 0).wait()

    colacc[...] = jnp.zeros_like(colacc)
    in_chunks(back_first, before=lambda c: ef_copy(c).wait_recv())
    exchange(zb, 1)
    receive(zb, 1)

    zero = jnp.zeros((S, L), F32)

    def image_first(i, sums):
        at, pad = rows_at(i), rows_at(i + 1)
        one, two = sums
        y = [None] * blocks
        for k in range(depth):
            near, value = sideways(zb, 1, i, k)
            for j in range(blocks):
                b = bb[lay[k], at, cut(j)]
                w = b - near[j]
                wb[lay[k], at, cut(j)] = w
                one = one + b * value[j]
                two = two + w * value[j]
                y[j] = w if k == 0 else w + gain[k - 1, at, cut(j)] * y[j]
                if k < last:
                    vb[lay[k], pad, cut(j)] = y[j] * inv[k, at, cut(j)]
                else:
                    f2[at, cut(j)] = y[j]
        return one, two

    def first_chunk(c, sums):
        sums = lax.fori_loop(0, per, lambda j, s: image_first(c * per + j, s), sums)
        f2_copy(c).start()
        return sums

    one, two = lax.fori_loop(0, chunks, first_chunk, (zero, zero))
    sum_begin(0, one, two)
    in_chunks(back_second, before=lambda c: f2_copy(c).wait_recv())
    exchange(vb, 2)
    sum_middle(0)
    receive(vb, 2)
    rho, power = sum_finish(0)
    alpha = rho / power
    step = jnp.broadcast_to(alpha, (S, L))

    def image_second(i, sums):
        at, pad = rows_at(i), rows_at(i + 1)
        one, two = sums
        for k in range(depth):
            near, value = sideways(vb, 2, i, k)
            for j in range(blocks):
                w = wb[lay[k], at, cut(j)]
                u = w - near[j]
                ut[lay[k], at, cut(j)] = u
                precond = zb[lay[k], pad, cut(j)] - step * value[j]
                one = one + (bb[lay[k], at, cut(j)] - step * w) * precond
                two = two + (w - step * u) * precond
        return one, two

    one, two = lax.fori_loop(0, tiles, image_second, (zero, zero))
    sum_begin(1, one, two)
    sum_middle(1)
    rho_next, curvature = sum_finish(1)
    ratio = rho_next / rho
    beta = rho_next / (curvature - ratio * rho_next / alpha)
    coef[0] = jnp.broadcast_to(alpha + beta * (1.0 + ratio), (S, L))
    coef[1] = jnp.broadcast_to(beta * alpha, (S, L))

    end_halo(0, (0, 2))
    end_halo(1, range(4))
    end_halo(2, range(4))
    pl.when(lower)(vm_copy.wait_send)

    def close(c, _):
        ef_copy(c).wait_send()
        f2_copy(c).wait_send()
        return 0

    lax.fori_loop(0, chunks, close, 0)
    sum_end(0)
    sum_end(1)


def finish(chunks, bb, zb, vb, wb, ut, coef, x_hbm, res_hbm, xb, resb, out_sem):
    depth, rows, width = bb.shape
    chunk_rows = rows // chunks
    on_z, on_v = coef[0], coef[1]

    def out_copies(c):
        at = pl.ds(c * chunk_rows, chunk_rows)
        return [pltpu.make_async_copy(xb.at[:, at], x_hbm.at[:, at], out_sem.at[0, c]),
                pltpu.make_async_copy(resb.at[:, at], res_hbm.at[:, at], out_sem.at[1, c])]

    for c in range(chunks):
        def tile(t, _):
            start = pl.multiple_of(c * chunk_rows + t * S, S)
            at, pad = pl.ds(start, S), pl.ds(pl.multiple_of(start + S, S), S)
            for k in range(depth):
                for j in range(width // L):
                    cut = pl.ds(j * L, L)
                    xb[k, at, cut] = on_z * zb[k, pad, cut] - on_v * vb[k, pad, cut]
                    resb[k, at, cut] = bb[k, at, cut] - on_z * wb[k, at, cut] + on_v * ut[k, at, cut]
            return 0

        lax.fori_loop(0, chunk_rows // S, tile, 0)
        for copy in out_copies(c):
            copy.start()
    for c in range(chunks):
        for copy in out_copies(c):
            copy.wait()


def solution(mesh):
    sizes = tuple(mesh.shape[name] for name in ("layer", "px", "py"))
    members, npx, npy = sizes
    assert members == 2

    def shards(*arrays):
        depth, rows, width = arrays[0].shape
        assert rows <= L and rows % S == 0 and width % L == 0 and depth >= 2
        chunks = max(c for c in (1, 2, 4) if (rows // S) % c == 0)
        peers = npx * npy
        full, plane, inner = (depth, rows, width), (rows, width), (depth - 1, rows, width)
        padded = (depth, rows + 2 * S, width)
        dma = pltpu.SemaphoreType.DMA

        def vmem(*shape, dtype=F32):
            return pltpu.VMEM(shape, dtype)

        scratch = [
            vmem(depth, rows + S, width), vmem(*full), vmem(*inner), vmem(*inner, dtype=jnp.int32), vmem(*full),
            vmem(*plane), vmem(*plane, dtype=jnp.int32),
            vmem(*inner), vmem(*inner), vmem(2, *plane), vmem(2, *plane), vmem(2, *plane), vmem(*plane), vmem(*plane),
            vmem(depth, S, width), vmem(depth, rows, L), vmem(depth, S, width), vmem(2, depth, S, L),
            vmem(3, 2, depth, width), vmem(3, 2, depth, width), vmem(3, 2, depth, L), vmem(3, 2, depth, L),
            vmem(2, 1, L), vmem(2, 1, L), vmem(2, 1, L), vmem(2, peers, 1, L),
            dma((6, chunks)), dma((2,)), dma((2,)), dma((2,)), dma((chunks, 2)), dma((chunks, 2)), dma((3, 4, 2)),
            dma((2, 2)), dma((2, 2)),
        ]
        anywhere = pl.BlockSpec(memory_space=pl.ANY)
        kept = pl.pallas_call(
            functools.partial(kernel, sizes, chunks),
            out_shape=(vmem(*full), vmem(*padded), vmem(*padded), vmem(*full), vmem(*full), vmem(2, S, L)),
            in_specs=[anywhere] * 6,
            out_specs=(pl.BlockSpec(memory_space=pltpu.VMEM),) * 6,
            scratch_shapes=scratch,
            compiler_params=pltpu.CompilerParams(
                collective_id=0, has_side_effects=True, vmem_limit_bytes=52 * 1024 * 1024),
            name="pcg",
        )(*arrays)
        return pl.pallas_call(
            functools.partial(finish, chunks),
            out_shape=(jax.ShapeDtypeStruct(full, F32), jax.ShapeDtypeStruct(full, F32)),
            in_specs=[pl.BlockSpec(memory_space=pltpu.VMEM)] * 6,
            out_specs=(anywhere,) * 2,
            scratch_shapes=[vmem(*full), vmem(*full), dma((2, chunks))],
            compiler_params=pltpu.CompilerParams(vmem_limit_bytes=8 * 1024 * 1024),
            name="finish",
        )(*kept)

    spec = P("layer", "px", "py")
    return jax.shard_map(shards, mesh=mesh, in_specs=(spec,) * 6, out_specs=(spec, spec), check_vma=False)
```

```python
import functools

import jax
import jax.numpy as jnp
from jax import lax
from jax.experimental import pallas as pl
from jax.experimental.pallas import tpu as pltpu
from jax.sharding import PartitionSpec as P

MESH = pl.DeviceIdType.MESH
S = 8
L = 128
F32 = jnp.float32


def kernel(sizes, chunks, b_hbm, r_hbm, c_hbm, via_hbm, mask_hbm, g_hbm, bb, zb, vb, wb, ut, coef,
           rb, cb, ub, mb, gb, vm, vmask, gain, inv, mid, ef, efo, f2, f2o,
           redge, cedge, spread_c, side, colacc, row_s, row_r, col_s, col_r, pair_s, pair_r, sum_s, sum_r,
           hello_sem, load_sem, edge_sem, vm_sem, ef_sem, f2_sem, halo_sem, pair_sem, sum_sem):
    members, npx, npy = sizes
    depth, rows, width = bb.shape
    tiles = rows // S
    per = tiles // chunks
    last = depth - 1
    blocks = width // L
    up = lax.axis_index("layer")
    px = lax.axis_index("px")
    py = lax.axis_index("py")
    lower = up == 0
    lay = [k + up * (last - 2 * k) for k in range(depth)]
    via_at = [k + up * (last - 1 - 2 * k) for k in range(last)]
    chunk_rows = per * S
    peers = npx * npy
    me = px * npy + py

    partner = (1 - up, px, py)
    above, below = (up, px - 1, py), (up, px + 1, py)
    left, right = (up, px, py - 1), (up, px, py + 1)

    row_r[...] = jnp.zeros_like(row_r)
    pair_s[...] = jnp.zeros_like(pair_s)
    col_r[...] = jnp.zeros_like(col_r)
    barrier = pltpu.get_barrier_semaphore()

    deep = max(d for d in range(1, npx + 1) if npx % d == 0 and d * d <= npx)
    wide = npx // deep
    in_deep = lax.rem(px, deep)
    mates = [(up, lax.rem(px + deep * o, npx), py) for o in range(1, wide)]
    mates += [(up, px - in_deep + lax.rem(in_deep + o, deep), py) for o in range(1, deep)]
    mates += [(up, px, lax.rem(py + o, npy)) for o in range(1, npy)]
    crossing = [] if deep == 1 else [
        (jnp.logical_and(in_deep == deep - 1, px < npx - 1), below), (jnp.logical_and(in_deep == 0, px > 0), above)]

    def hello(t):
        for device in mates:
            pl.semaphore_signal(hello_sem.at[t], inc=1, device_id=device, device_id_type=MESH)

    def heard(t):
        pl.semaphore_wait(hello_sem.at[t], len(mates))

    pl.semaphore_signal(barrier, inc=1, device_id=partner, device_id_type=MESH)
    for device in mates:
        pl.semaphore_signal(barrier, inc=1, device_id=device, device_id_type=MESH)
    for exists, device in crossing:
        @pl.when(exists)
        def _():
            pl.semaphore_signal(barrier, inc=1, device_id=device, device_id_type=MESH)

    edge_loads = [
        pltpu.make_async_copy(r_hbm.at[:, pl.ds(rows - S, S)], redge, edge_sem.at[0]),
        pltpu.make_async_copy(c_hbm.at[:, :, pl.ds(width - L, L)], cedge, edge_sem.at[1]),
    ]
    for copy in edge_loads:
        copy.start()

    def chunk_at(c, ahead=0):
        start = c * chunk_rows + ahead
        return pl.ds(start if isinstance(start, int) else pl.multiple_of(start, S), chunk_rows)

    def top(c):
        at = chunk_at(c)
        return [pltpu.make_async_copy(via_hbm.at[last, at], vm.at[at], load_sem.at[c]),
                pltpu.make_async_copy(mask_hbm.at[last, at], vmask.at[at], load_sem.at[c])]

    def loads(c):
        at = chunk_at(c)
        inner = pl.ds(0, last)
        pairs = [(c_hbm.at[:, at], cb.at[:, at]),
                 (g_hbm.at[:, at], gb.at[:, at]), (via_hbm.at[inner, at], ub.at[:, at]),
                 (mask_hbm.at[inner, at], mb.at[:, at]), (b_hbm.at[:, at], bb.at[:, at])]
        return [pltpu.make_async_copy(src, dst, load_sem.at[c]) for src, dst in pairs]

    def row_load(c):
        start = c * chunk_rows - (S if c == 1 else 0)
        size = chunk_rows + (S if c == 1 else -S if c == 0 else 0)
        return pltpu.make_async_copy(
            r_hbm.at[:, pl.ds(start, size)], rb.at[:, pl.ds(start + S, size)], load_sem.at[c])

    def start_loads(c):
        row_load(c).start()
        for copy in loads(c):
            copy.start()

        @pl.when(lower)
        def _():
            for copy in top(c):
                copy.start()

    start_loads(1 % chunks)

    lane = lax.broadcasted_iota(jnp.int32, (S, L), 1)
    sub = lax.broadcasted_iota(jnp.int32, (S, L), 0)
    first_lane, final_lane = lane == 0, lane == L - 1
    first_sub, final_sub = sub == 0, sub == S - 1

    def remote(src, dst, sems, device):
        return pltpu.make_async_remote_copy(
            src_ref=src, dst_ref=dst, send_sem=sems.at[0], recv_sem=sems.at[1],
            device_id=device, device_id_type=MESH)

    def exchanges(trip):
        def one(e, src, dst, device):
            return remote(src, dst, halo_sem.at[trip % 2, e], device)

        down_up = [
            (px < npx - 1, px > 0, one(0, row_s.at[trip, 0], row_r.at[trip, 0], below)),
            (px > 0, px < npx - 1, one(1, row_s.at[trip, 1], row_r.at[trip, 1], above)),
        ]
        for part in range(2):
            sent, got = col_s.at[trip, part], col_r.at[trip, part]
            down_up.append((py < npy - 1, py > 0, one(2 + 2 * part, sent.at[0], got.at[0], right)))
            down_up.append((py > 0, py < npy - 1, one(3 + 2 * part, sent.at[1], got.at[1], left)))
        return down_up

    def send_halo(trip, which):
        for e in which:
            sends, _, copy = exchanges(trip)[e]
            pl.when(sends)(copy.start)

    def take_halo(trip, which):
        for e in which:
            sends, takes, copy = exchanges(trip)[e]
            pl.when(takes)(copy.wait_recv)

    def end_halo(trip, which):
        for e in which:
            sends, _, copy = exchanges(trip)[e]
            pl.when(sends)(copy.wait_send)

    for copy in edge_loads:
        copy.wait()
    for c in range(1, chunks):
        start_loads((1 + c) % chunks)
    for k in range(depth):
        row_s[0, 0, k:k + 1, :] = redge[lay[k], S - 1:S, :]
        acc = jnp.zeros((S, L), F32)
        for i in range(tiles):
            edge = jnp.broadcast_to(cedge[lay[k], i * S:(i + 1) * S, L - 1:L], (S, L))
            acc = jnp.where(lane == sub + i * S, edge, acc)
        col_s[0, 0, 0, k:k + 1, :] = jnp.sum(acc, axis=0, keepdims=True)

    pl.semaphore_wait(barrier, 1 + len(mates) + sum(exists.astype(jnp.int32) for exists, _ in crossing))
    send_halo(0, (0, 2))
    hello(0)
    take_halo(0, (2,))

    def spread(ref):
        for k in range(depth):
            both = jnp.concatenate([jnp.broadcast_to(ref[side_of, k:k + 1, :], (L // 2, L)) for side_of in range(2)], axis=0)
            spread_c[k] = jnp.transpose(both)[:rows]

    def rows_at(i):
        return pl.ds(pl.multiple_of(i * S, S), S)

    def cut(j):
        return pl.ds(j * L, L)

    def next_row(now, after):
        return pltpu.roll(jnp.where(first_sub, after, now), S - 1, 0)

    def prev_row(now, before):
        return pltpu.roll(jnp.where(final_sub, before, now), 1, 0)

    def from_left(parts, edge):
        turned = [pltpu.roll(p, 1, 1) for p in parts]
        return [jnp.where(first_lane, turned[j - 1] if j else edge, turned[j]) for j in range(blocks)]

    def factor_tile(i):
        at, pad = rows_at(i), rows_at(i + 1)
        coupling, g, y = [None] * blocks, [None] * blocks, [None] * blocks
        for k in range(depth):
            edge = spread_c[k, at, :]
            c = [cb[lay[k], at, cut(j)] for j in range(blocks)]
            c_left = from_left(c, edge)
            for j in range(blocks):
                r = rb[lay[k], pad, cut(j)]
                d = gb[lay[k], at, cut(j)] + r + prev_row(r, rb[lay[k], at, cut(j)]) + c[j] + c_left[j]
                rhs = bb[lay[k], at, cut(j)]
                if k:
                    d = d + coupling[j] - coupling[j] * g[j]
                    rhs = rhs + g[j] * y[j]
                y[j] = rhs
                if k < last:
                    coupling[j] = ub[via_at[k], at, cut(j)] * mb[via_at[k], at, cut(j)].astype(F32)
                    inverse = 1.0 / (d + coupling[j])
                    g[j] = coupling[j] * inverse
                    gain[k, at, cut(j)] = g[j]
                    inv[k, at, cut(j)] = inverse
                    zb[lay[k], pad, cut(j)] = rhs * inverse
                else:
                    ef[0, at, cut(j)] = d
                    ef[1, at, cut(j)] = rhs

    def to_partner(src, dst, sems, c):
        return pltpu.make_async_remote_copy(
            src_ref=src, dst_ref=dst, send_sem=sems.at[chunks], recv_sem=sems.at[c],
            device_id=partner, device_id_type=MESH)

    def all_sent(ref, sems):
        pltpu.make_async_copy(ref, ref, sems.at[chunks]).wait()

    def vm_copy(c):
        return to_partner(vm.at[chunk_at(c)], vm.at[chunk_at(c)], vm_sem, c)

    def ef_copy(c):
        return to_partner(ef.at[:, chunk_at(c)], efo.at[:, chunk_at(c)], ef_sem, c)

    def f2_copy(c):
        return to_partner(f2.at[chunk_at(c)], f2o.at[chunk_at(c)], f2_sem, c)

    def low_last(q):
        return lax.rem(q + 1, chunks)

    def high_last(q):
        return jnp.where(q < chunks - 2, q + 1, jnp.where(q == chunks - 2, 0, chunks - 1))

    def in_chunks(tile, order=low_last, before=None, after=None):
        def chunk(q, _):
            c = order(q)
            if before is not None:
                before(c)

            def one(j, _):
                tile(c * per + j)
                return 0

            lax.fori_loop(0, per, one, 0)
            if after is not None:
                after(c)
            return 0

        lax.fori_loop(0, chunks, chunk, 0)

    def wait_loads(c):
        for one in range(chunks):
            pl.when(c == one)(row_load(one).wait)
        for copy in loads(c):
            copy.wait()

        @pl.when(c == 0)
        def _():
            take_halo(0, (0,))
            for k in range(depth):
                rb[lay[k], S - 1:S, :] = row_r[0, 0, k:k + 1, :]

        @pl.when(lower)
        def _():
            for copy in top(c):
                copy.wait()

        @pl.when(lower)
        def _():
            def times(j, _):
                at = rows_at(c * per + j)
                for b in range(blocks):
                    vm[at, cut(b)] = vm[at, cut(b)] * vmask[at, cut(b)].astype(F32)
                return 0

            lax.fori_loop(0, per, times, 0)
            vm_copy(c).start()

    spread(col_r.at[0, 0])
    in_chunks(factor_tile, before=wait_loads, after=lambda c: ef_copy(c).start())

    def back(field, i, own):
        at, pad = rows_at(i), rows_at(i + 1)
        mine = lane == sub + i * S
        value = own
        for k in range(last, -1, -1):
            for j in range(blocks):
                if k < last:
                    value[j] = field[lay[k], pad, cut(j)] + gain[k, at, cut(j)] * value[j]
                field[lay[k], pad, cut(j)] = value[j]
            first = jnp.broadcast_to(value[0][:, 0:1], (S, L))
            final = jnp.broadcast_to(value[blocks - 1][:, L - 1:L], (S, L))
            colacc[0, k] = jnp.where(mine, final, colacc[0, k])
            colacc[1, k] = jnp.where(mine, first, colacc[1, k])

    def back_first(i):
        at = rows_at(i)
        value = []
        for j in range(blocks):
            e, f = ef[0, at, cut(j)], ef[1, at, cut(j)]
            eo, fo = efo[0, at, cut(j)], efo[1, at, cut(j)]
            v = vm[at, cut(j)]
            shared = 1.0 / (e * eo + v * (e + eo))
            own, cross = (eo + v) * shared, v * shared
            mid[0, at, cut(j)] = own
            mid[1, at, cut(j)] = cross
            value.append(own * f + cross * fo)
        back(zb, i, value)

    def back_second(i):
        at = rows_at(i)
        back(vb, i, [mid[0, at, cut(j)] * f2[at, cut(j)] + mid[1, at, cut(j)] * f2o[at, cut(j)] for j in range(blocks)])

    def send_part(field, trip, part, side_of):
        at = S if side_of else rows + S - 1
        for k in range(depth):
            row_s[trip, side_of, k:k + 1, :] = field[lay[k], at:at + 1, :]
            final = jnp.sum(colacc[0, k], axis=0, keepdims=True)
            col_s[trip, part, 0, k:k + 1, :] = final * col_s[0, 0, 0, k:k + 1, :]
            col_s[trip, part, 1, k:k + 1, :] = jnp.sum(colacc[1, k], axis=0, keepdims=True)
        send_halo(trip, (side_of, 2 + 2 * part, 3 + 2 * part))

    def receive_row(field, trip, side_of):
        at = rows + S if side_of else S - 1
        take_halo(trip, (side_of,))
        for k in range(depth):
            field[lay[k], at:at + 1, :] = row_r[trip, side_of, k:k + 1, :]

    def low_tiles(p):
        return jnp.where(p < tiles - per - 1, p + per, jnp.where(p < tiles - 1, tiles - 2 - p, tiles - 1))

    def high_tiles(p):
        return lax.rem(p + 1, tiles)

    def sideways(field, i, k):
        at, pad, ahead = rows_at(i), rows_at(i + 1), rows_at(i + 2)
        value = [field[lay[k], pad, cut(j)] for j in range(blocks)]
        c = [cb[lay[k], at, cut(j)] for j in range(blocks)]
        outside = spread_c[k, at, :]
        turned = [(pltpu.roll(c[j] * value[j], 1, 1), pltpu.roll(value[j], L - 1, 1)) for j in range(blocks)]
        to_right = [jnp.where(first_lane, turned[j - 1][0] if j else outside, turned[j][0]) for j in range(blocks)]
        beside = [jnp.where(final_lane, turned[j + 1][1] if j < blocks - 1 else outside, turned[j][1])
                  for j in range(blocks)]
        for j in range(blocks):
            r = rb[lay[k], pad, cut(j)]
            down = r * value[j]
            before = rb[lay[k], at, cut(j)] * field[lay[k], at, cut(j)]
            term = r * next_row(value[j], field[lay[k], ahead, cut(j)]) + prev_row(down, before)
            side[k, :, cut(j)] = term + (c[j] * beside[j] + to_right[j])

    def first_sides(field, trip):
        take_halo(trip, (2, 3))
        spread(col_r.at[trip, 0])
        for k in range(depth):
            sideways(field, per if trip == 1 else 1, k)

    def take_columns(trip):
        take_halo(trip, (4, 5))
        spread(col_r.at[trip, 1])

    def images(field, trip, order, begin, carry, after=None):
        needs = [(tiles - per - 1, lambda: take_columns(trip)),
                 (tiles - 2 if trip == 1 else tiles - 1, lambda: receive_row(field, trip, 0)),
                 (tiles - 1 if trip == 1 else tiles - 2, lambda: receive_row(field, trip, 1))]

        def chunk(q, carry):
            for j in range(per):
                for place, take in needs:
                    if (place - 1) % per == j:
                        pl.when(q == (place - 1) // per)(take)
                position = q * per + j
                use, ahead = begin(order(position)), order(lax.rem(position + 1, tiles))
                for k in range(depth):
                    carry = use(k, [side[k, :, cut(b)] for b in range(blocks)], carry)
                    sideways(field, ahead, k)
            if after is not None:
                after(q)
            return carry

        return lax.fori_loop(0, chunks, chunk, carry)

    def down(total):
        return jnp.sum(total, axis=0, keepdims=True)

    def across(total):
        return jnp.sum(total, axis=1, keepdims=True)

    def pair_copy(slot):
        return remote(pair_s.at[slot], pair_r.at[slot], pair_sem.at[slot], partner)

    def pair_begin(slot, totals):
        for q, total in enumerate(totals):
            pair_s[slot, q:q + 1, :] = down(total)
        pair_copy(slot).start()

    def pair_finish(slot):
        pair_copy(slot).wait_recv()
        return across(pair_s[slot] + pair_r[slot])

    def sum_copies():
        def way(o, n):
            return min(o, n - o)

        offsets = [(a, b) for a in range(npx) for b in range(npy) if a or b]
        offsets.sort(key=lambda o: -way(o[0] // deep, wide) - way(o[0] % deep, deep) - way(o[1], npy))
        to_x, to_y = [lax.rem(px + a, npx) for a in range(npx)], [lax.rem(py + b, npy) for b in range(npy)]
        return [remote(sum_s, sum_r.at[me], sum_sem, (up, to_x[a], to_y[b])) for a, b in offsets]

    def sum_bytes(end):
        part = sum_r.at[pl.ds(0, peers - 1)]
        return pltpu.make_async_copy(part, part, sum_sem.at[end])

    colacc[...] = jnp.zeros_like(colacc)

    def wait_middle(c):
        ef_copy(c).wait_recv()
        pl.when(up == 1)(vm_copy(c).wait_recv)

    in_chunks(back_first, before=wait_middle,
              after=lambda c: pl.when(c == chunks - 1)(lambda: send_part(zb, 1, 0, 0)))
    send_part(zb, 1, 1, 1)
    heard(0)
    hello(1)

    zero = jnp.zeros((S, L), F32)

    def image_first(i):
        at, pad = rows_at(i), rows_at(i + 1)
        y = [None] * blocks

        def use(k, terms, sums):
            one, two = sums
            for j in range(blocks):
                b, value = bb[lay[k], at, cut(j)], zb[lay[k], pad, cut(j)]
                w = b - terms[j]
                wb[lay[k], at, cut(j)] = w
                one = one + b * value
                two = two + w * value
                y[j] = w if k == 0 else w + gain[k - 1, at, cut(j)] * y[j]
                if k < last:
                    vb[lay[k], pad, cut(j)] = y[j] * inv[k, at, cut(j)]
                else:
                    f2[at, cut(j)] = y[j]
            return one, two

        return use

    first_sides(zb, 1)
    one, two = images(zb, 1, low_tiles, image_first, (zero, zero),
                      after=lambda q: pl.when(q < chunks - 2)(lambda: f2_copy(q + 1).start()))
    f2_copy(0).start()
    f2_copy(chunks - 1).start()
    pair_begin(0, (one, two))
    end_halo(0, (0, 2))
    in_chunks(back_second, order=high_last, before=lambda c: f2_copy(c).wait_recv(),
              after=lambda c: pl.when(c == 0)(lambda: send_part(vb, 2, 0, 1)))
    send_part(vb, 2, 1, 0)
    here = pair_finish(0)
    rho_here, power_here = here[0:1], here[1:2]
    known = power_here > 0.0
    guess = jnp.where(known, jnp.clip(rho_here / jnp.where(known, power_here, 1.0), 0.25, 256.0), 1.0)
    step = jnp.broadcast_to(guess, (S, L))
    first_sides(vb, 2)

    def image_second(i):
        at, pad = rows_at(i), rows_at(i + 1)

        def use(k, terms, sums):
            rp, wv, qp, uv, uz = sums
            for j in range(blocks):
                w, v, z = wb[lay[k], at, cut(j)], vb[lay[k], pad, cut(j)], zb[lay[k], pad, cut(j)]
                u = w - terms[j]
                ut[lay[k], at, cut(j)] = u
                p = z - step * v
                rp = rp + (bb[lay[k], at, cut(j)] - step * w) * p
                wv = wv + w * v
                qp = qp + (w - step * u) * p
                uv = uv + u * v
                uz = uz + u * z
            return rp, wv, qp, uv, uz

        return use

    sums = images(vb, 2, high_tiles, image_second, (zero,) * 5)
    pair_begin(1, sums)
    heard(1)
    here = pair_finish(1)
    rp, wv, qp, uv, uz = [here[q:q + 1] for q in range(5)]
    entries = [rp, qp, power_here - guess * wv, 0.5 * (wv + uz) - guess * uv, wv, uv, guess, guess, rho_here, power_here]
    row = jnp.zeros((1, L), F32)
    for q, entry in enumerate(entries):
        row = jnp.where(lane[0:1] == q, entry, row)
    sum_s[...] = row
    sum_r[me] = row

    for copy in sum_copies():
        copy.start()

    end_halo(1, range(6))
    end_halo(2, range(6))
    all_sent(ef, ef_sem)
    all_sent(f2, f2_sem)
    pl.when(lower)(lambda: all_sent(vm, vm_sem))
    pair_copy(0).wait_send()
    pair_copy(1).wait_send()

    def pick(total, q):
        return across(jnp.where(lane[0:1] == q, total, 0.0))

    sum_bytes(1).wait()
    rows_all = sum_r[...].reshape(peers, L)
    total = down(rows_all)
    rho = pick(total, 8)
    alpha = rho / pick(total, 9)
    off = alpha - pltpu.roll(rows_all, L - 6, 1)
    total = down(rows_all - off * (2.0 * pltpu.roll(rows_all, L - 2, 1) - off * pltpu.roll(rows_all, L - 4, 1)))
    rho_next, curvature = pick(total, 0), pick(total, 1)
    ratio = rho_next / rho
    beta = rho_next / (curvature - ratio * rho_next / alpha)
    coef[0] = jnp.broadcast_to(alpha + beta * (1.0 + ratio), (S, L))
    coef[1] = jnp.broadcast_to(beta * alpha, (S, L))

    sum_bytes(0).wait()


def finish(chunks, bb, zb, vb, wb, ut, coef, x_hbm, res_hbm, xb, resb, out_sem):
    depth, rows, width = bb.shape
    chunk_rows = rows // chunks
    on_z, on_v = coef[0], coef[1]

    def out_copies(c):
        at = pl.ds(c * chunk_rows, chunk_rows)
        return [pltpu.make_async_copy(xb.at[:, at], x_hbm.at[:, at], out_sem.at[0, c]),
                pltpu.make_async_copy(resb.at[:, at], res_hbm.at[:, at], out_sem.at[1, c])]

    for c in range(chunks):
        def tile(t, _):
            start = pl.multiple_of(c * chunk_rows + t * S, S)
            at, pad = pl.ds(start, S), pl.ds(pl.multiple_of(start + S, S), S)
            for k in range(depth):
                for j in range(width // L):
                    cut = pl.ds(j * L, L)
                    xb[k, at, cut] = on_z * zb[k, pad, cut] - on_v * vb[k, pad, cut]
                    resb[k, at, cut] = bb[k, at, cut] - on_z * wb[k, at, cut] + on_v * ut[k, at, cut]
            return 0

        lax.fori_loop(0, chunk_rows // S, tile, 0)
        for copy in out_copies(c):
            copy.start()
    for c in range(chunks):
        for copy in out_copies(c):
            copy.wait()


def solution(mesh):
    sizes = tuple(mesh.shape[name] for name in ("layer", "px", "py"))
    members, npx, npy = sizes
    assert members == 2

    def shards(*arrays):
        depth, rows, width = arrays[0].shape
        assert rows <= L and rows % S == 0 and width % L == 0 and depth >= 2
        chunks = max(c for c in (2, 4) if (rows // S) % c == 0)
        peers = npx * npy
        full, plane, inner = (depth, rows, width), (rows, width), (depth - 1, rows, width)
        padded = (depth, rows + 2 * S, width)
        dma = pltpu.SemaphoreType.DMA

        def vmem(*shape, dtype=F32):
            return pltpu.VMEM(shape, dtype)

        scratch = [
            vmem(depth, rows + S, width), vmem(*full), vmem(*inner), vmem(*inner, dtype=jnp.int32), vmem(*full),
            vmem(*plane), vmem(*plane, dtype=jnp.int32),
            vmem(*inner), vmem(*inner), vmem(2, *plane), vmem(2, *plane), vmem(2, *plane), vmem(*plane), vmem(*plane),
            vmem(depth, S, width), vmem(depth, rows, L), vmem(depth, rows, L), vmem(depth, S, width), vmem(2, depth, S, L),
            vmem(3, 2, depth, width), vmem(3, 2, depth, width), vmem(3, 2, 2, depth, L), vmem(3, 2, 2, depth, L),
            vmem(2, S, L), vmem(2, S, L), vmem(1, L), vmem(peers, 1, L),
            pltpu.SemaphoreType.REGULAR((2,)),
            dma((chunks,)), dma((2,)), dma((chunks + 1,)), dma((chunks + 1,)), dma((chunks + 1,)), dma((2, 6, 2)),
            dma((2, 2)), dma((2,)),
        ]
        anywhere = pl.BlockSpec(memory_space=pl.ANY)
        kept = pl.pallas_call(
            functools.partial(kernel, sizes, chunks),
            out_shape=(vmem(*full), vmem(*padded), vmem(*padded), vmem(*full), vmem(*full), vmem(2, S, L)),
            in_specs=[anywhere] * 6,
            out_specs=(pl.BlockSpec(memory_space=pltpu.VMEM),) * 6,
            scratch_shapes=scratch,
            compiler_params=pltpu.CompilerParams(
                collective_id=0, has_side_effects=True, vmem_limit_bytes=52 * 1024 * 1024),
            name="pcg",
        )(*arrays)
        return pl.pallas_call(
            functools.partial(finish, chunks),
            out_shape=(jax.ShapeDtypeStruct(full, F32), jax.ShapeDtypeStruct(full, F32)),
            in_specs=[pl.BlockSpec(memory_space=pltpu.VMEM)] * 6,
            out_specs=(anywhere,) * 2,
            scratch_shapes=[vmem(*full), vmem(*full), dma((2, chunks))],
            compiler_params=pltpu.CompilerParams(vmem_limit_bytes=8 * 1024 * 1024),
            name="finish",
        )(*kept)

    spec = P("layer", "px", "py")
    return jax.shard_map(shards, mesh=mesh, in_specs=(spec,) * 6, out_specs=(spec, spec), check_vma=False)
```

```python
import functools

import jax
import jax.numpy as jnp
from jax import lax
from jax.experimental import pallas as pl
from jax.experimental.pallas import tpu as pltpu
from jax.sharding import PartitionSpec as P

MESH = pl.DeviceIdType.MESH
S = 8
L = 128
F32 = jnp.float32


def kernel(sizes, chunks, b_hbm, r_hbm, c_hbm, via_hbm, mask_hbm, g_hbm, bb, zb, vb, wb, ut, coef,
           rb, cb, ub, mb, gb, vm, vmask, gain, inv, mid, ef, efo, f2, f2o,
           redge, cedge, spread_c, side, colacc, row_s, row_r, col_s, col_r, pair_s, pair_r, sum_s, sum_r,
           hello_sem, load_sem, edge_sem, vm_sem, ef_sem, f2_sem, halo_sem, pair_sem, sum_sem):
    members, npx, npy = sizes
    depth, rows, width = bb.shape
    tiles = rows // S
    per = tiles // chunks
    last = depth - 1
    blocks = width // L
    up = lax.axis_index("layer")
    px = lax.axis_index("px")
    py = lax.axis_index("py")
    lower = up == 0
    lay = [k + up * (last - 2 * k) for k in range(depth)]
    via_at = [k + up * (last - 1 - 2 * k) for k in range(last)]
    chunk_rows = per * S
    peers = npx * npy
    me = px * npy + py

    partner = (1 - up, px, py)
    above, below = (up, px - 1, py), (up, px + 1, py)
    left, right = (up, px, py - 1), (up, px, py + 1)

    row_r[...] = jnp.zeros_like(row_r)
    pair_s[...] = jnp.zeros_like(pair_s)
    col_r[...] = jnp.zeros_like(col_r)
    barrier = pltpu.get_barrier_semaphore()

    deep = max(d for d in range(1, npx + 1) if npx % d == 0 and d * d <= npx)
    wide = npx // deep
    in_deep = lax.rem(px, deep)
    across_wide = [(up, lax.rem(px + deep * o, npx), py) for o in range(1, wide)]
    along_deep = [(up, px - in_deep + lax.rem(in_deep + o, deep), py) for o in range(1, deep)]
    along_py = [(up, px, lax.rem(py + o, npy)) for o in range(1, npy)]
    mates = [(None, device) for device in across_wide + along_deep + along_py]

    def within(reach):
        found = []
        for o in [o for r in range(1, reach + 1) for o in (-r, r)]:
            if abs(o) < deep:
                found.append((jnp.logical_and(in_deep + o >= 0, in_deep + o < deep), (up, px + o, py)))
            if abs(o) < npy:
                found.append((jnp.logical_and(py + o >= 0, py + o < npy), (up, px, py + o)))
        return found

    crossing = [] if deep == 1 else [
        (jnp.logical_and(in_deep == deep - 1, px < npx - 1), below), (jnp.logical_and(in_deep == 0, px > 0), above)]
    near = [(None, partner)] + [(None, device) for device in across_wide] + within(1) + crossing
    rounds, reach = [], 1
    while reach < max(deep, npy) - 1:
        rounds.append(within(reach))
        reach *= 2
    rounds += [mates, mates]
    assert len(rounds) <= hello_sem.shape[0]

    def greet(sem, targets):
        for exists, device in targets:
            def signal(device=device):
                pl.semaphore_signal(sem, inc=1, device_id=device, device_id_type=MESH)

            signal() if exists is None else pl.when(exists)(signal)

    def count(targets):
        return sum(1 if exists is None else exists.astype(jnp.int32) for exists, _ in targets)

    def hello(t):
        greet(hello_sem.at[t], rounds[t])

    def heard(t):
        if t < len(rounds):
            pl.semaphore_wait(hello_sem.at[t], count(rounds[t]))
        if t + 1 < len(rounds):
            hello(t + 1)

    greet(barrier, near)

    edge_loads = [
        pltpu.make_async_copy(r_hbm.at[:, pl.ds(rows - S, S)], redge, edge_sem.at[0]),
        pltpu.make_async_copy(c_hbm.at[:, :, pl.ds(width - L, L)], cedge, edge_sem.at[1]),
    ]
    for copy in edge_loads:
        copy.start()

    def chunk_at(c, ahead=0):
        start = c * chunk_rows + ahead
        return pl.ds(start if isinstance(start, int) else pl.multiple_of(start, S), chunk_rows)

    def top(c):
        at = chunk_at(c)
        return [pltpu.make_async_copy(via_hbm.at[last, at], vm.at[at], load_sem.at[c]),
                pltpu.make_async_copy(mask_hbm.at[last, at], vmask.at[at], load_sem.at[c])]

    def loads(c):
        at = chunk_at(c)
        inner = pl.ds(0, last)
        pairs = [(c_hbm.at[:, at], cb.at[:, at]),
                 (g_hbm.at[:, at], gb.at[:, at]), (via_hbm.at[inner, at], ub.at[:, at]),
                 (mask_hbm.at[inner, at], mb.at[:, at]), (b_hbm.at[:, at], bb.at[:, at])]
        return [pltpu.make_async_copy(src, dst, load_sem.at[c]) for src, dst in pairs]

    def row_load(c):
        start = c * chunk_rows - (S if c == 1 else 0)
        size = chunk_rows + (S if c == 1 else -S if c == 0 else 0)
        return pltpu.make_async_copy(
            r_hbm.at[:, pl.ds(start, size)], rb.at[:, pl.ds(start + S, size)], load_sem.at[c])

    def start_loads(c):
        row_load(c).start()
        for copy in loads(c):
            copy.start()

        @pl.when(lower)
        def _():
            for copy in top(c):
                copy.start()

    start_loads(1 % chunks)

    lane = lax.broadcasted_iota(jnp.int32, (S, L), 1)
    sub = lax.broadcasted_iota(jnp.int32, (S, L), 0)
    first_lane, final_lane = lane == 0, lane == L - 1
    first_sub, final_sub = sub == 0, sub == S - 1

    def remote(src, dst, sems, device):
        return pltpu.make_async_remote_copy(
            src_ref=src, dst_ref=dst, send_sem=sems.at[0], recv_sem=sems.at[1],
            device_id=device, device_id_type=MESH)

    def exchanges(trip):
        def one(e, src, dst, device):
            return pltpu.make_async_remote_copy(
                src_ref=src, dst_ref=dst, send_sem=halo_sem.at[2, 0], recv_sem=halo_sem.at[trip % 2, e],
                device_id=device, device_id_type=MESH)

        down_up = [
            (px < npx - 1, px > 0, one(0, row_s.at[trip, 0], row_r.at[trip, 0], below)),
            (px > 0, px < npx - 1, one(1, row_s.at[trip, 1], row_r.at[trip, 1], above)),
        ]
        for part in range(2):
            sent, got = col_s.at[trip, part], col_r.at[trip, part]
            down_up.append((py < npy - 1, py > 0, one(2 + 2 * part, sent.at[0], got.at[0], right)))
            down_up.append((py > 0, py < npy - 1, one(3 + 2 * part, sent.at[1], got.at[1], left)))
        return down_up

    def send_halo(trip, which):
        for e in which:
            sends, _, copy = exchanges(trip)[e]
            pl.when(sends)(copy.start)

    def take_halo(trip, which):
        for e in which:
            sends, takes, copy = exchanges(trip)[e]
            pl.when(takes)(copy.wait_recv)

    def end_halo(trip, which):
        for e in which:
            sends, _, copy = exchanges(trip)[e]
            pl.when(sends)(copy.wait_send)

    for copy in edge_loads:
        copy.wait()
    for c in range(1, chunks):
        start_loads((1 + c) % chunks)
    for k in range(depth):
        row_s[0, 0, k:k + 1, :] = redge[lay[k], S - 1:S, :]
        acc = jnp.zeros((S, L), F32)
        for i in range(tiles):
            edge = jnp.broadcast_to(cedge[lay[k], i * S:(i + 1) * S, L - 1:L], (S, L))
            acc = jnp.where(lane == sub + i * S, edge, acc)
        col_s[0, 0, 0, k:k + 1, :] = jnp.sum(acc, axis=0, keepdims=True)

    pl.semaphore_wait(barrier, count(near))
    send_halo(0, (0, 2))
    hello(0)
    take_halo(0, (2,))

    def spread(ref):
        for k in range(depth):
            both = jnp.concatenate([jnp.broadcast_to(ref[side_of, k:k + 1, :], (L // 2, L)) for side_of in range(2)], axis=0)
            spread_c[k] = jnp.transpose(both)[:rows]

    def rows_at(i):
        return pl.ds(pl.multiple_of(i * S, S), S)

    def cut(j):
        return pl.ds(j * L, L)

    def next_row(now, after):
        return pltpu.roll(jnp.where(first_sub, after, now), S - 1, 0)

    def prev_row(now, before):
        return pltpu.roll(jnp.where(final_sub, before, now), 1, 0)

    def from_left(parts, edge):
        turned = [pltpu.roll(p, 1, 1) for p in parts]
        return [jnp.where(first_lane, turned[j - 1] if j else edge, turned[j]) for j in range(blocks)]

    def factor_tile(i):
        at, pad = rows_at(i), rows_at(i + 1)
        coupling, g, y = [None] * blocks, [None] * blocks, [None] * blocks
        for k in range(depth):
            edge = spread_c[k, at, :]
            c = [cb[lay[k], at, cut(j)] for j in range(blocks)]
            c_left = from_left(c, edge)
            for j in range(blocks):
                r = rb[lay[k], pad, cut(j)]
                d = gb[lay[k], at, cut(j)] + r + prev_row(r, rb[lay[k], at, cut(j)]) + c[j] + c_left[j]
                rhs = bb[lay[k], at, cut(j)]
                if k:
                    d = d + coupling[j] - coupling[j] * g[j]
                    rhs = rhs + g[j] * y[j]
                y[j] = rhs
                if k < last:
                    coupling[j] = ub[via_at[k], at, cut(j)] * mb[via_at[k], at, cut(j)].astype(F32)
                    inverse = 1.0 / (d + coupling[j])
                    g[j] = coupling[j] * inverse
                    gain[k, at, cut(j)] = g[j]
                    inv[k, at, cut(j)] = inverse
                    zb[lay[k], pad, cut(j)] = rhs * inverse
                else:
                    ef[0, at, cut(j)] = d
                    ef[1, at, cut(j)] = rhs

    def to_partner(src, dst, sems, c):
        return pltpu.make_async_remote_copy(
            src_ref=src, dst_ref=dst, send_sem=sems.at[chunks], recv_sem=sems.at[c],
            device_id=partner, device_id_type=MESH)

    def all_sent(ref, sems):
        pltpu.make_async_copy(ref, ref, sems.at[chunks]).wait()

    def vm_copy(c):
        return to_partner(vm.at[chunk_at(c)], vm.at[chunk_at(c)], vm_sem, c)

    def ef_copy(c):
        return to_partner(ef.at[:, chunk_at(c)], efo.at[:, chunk_at(c)], ef_sem, c)

    def f2_copy(c):
        return to_partner(f2.at[chunk_at(c)], f2o.at[chunk_at(c)], f2_sem, c)

    def low_last(q):
        return lax.rem(q + 1, chunks)

    def high_last(q):
        return jnp.where(q < chunks - 2, q + 1, jnp.where(q == chunks - 2, 0, chunks - 1))

    def in_chunks(tile, order=low_last, before=None, after=None):
        def chunk(q, _):
            c = order(q)
            if before is not None:
                before(c)

            def one(j, _):
                tile(c * per + j)
                return 0

            lax.fori_loop(0, per, one, 0)
            if after is not None:
                after(c)
            return 0

        lax.fori_loop(0, chunks, chunk, 0)

    def wait_loads(c):
        for one in range(chunks):
            pl.when(c == one)(row_load(one).wait)
        for copy in loads(c):
            copy.wait()

        @pl.when(c == 0)
        def _():
            take_halo(0, (0,))
            for k in range(depth):
                rb[lay[k], S - 1:S, :] = row_r[0, 0, k:k + 1, :]

        @pl.when(lower)
        def _():
            for copy in top(c):
                copy.wait()

        @pl.when(lower)
        def _():
            def times(j, _):
                at = rows_at(c * per + j)
                for b in range(blocks):
                    vm[at, cut(b)] = vm[at, cut(b)] * vmask[at, cut(b)].astype(F32)
                return 0

            lax.fori_loop(0, per, times, 0)
            vm_copy(c).start()

    spread(col_r.at[0, 0])
    in_chunks(factor_tile, before=wait_loads, after=lambda c: ef_copy(c).start())

    def back(field, i, own):
        at, pad = rows_at(i), rows_at(i + 1)
        mine = lane == sub + i * S
        value = own
        for k in range(last, -1, -1):
            for j in range(blocks):
                if k < last:
                    value[j] = field[lay[k], pad, cut(j)] + gain[k, at, cut(j)] * value[j]
                field[lay[k], pad, cut(j)] = value[j]
            first = jnp.broadcast_to(value[0][:, 0:1], (S, L))
            final = jnp.broadcast_to(value[blocks - 1][:, L - 1:L], (S, L))
            colacc[0, k] = jnp.where(mine, final, colacc[0, k])
            colacc[1, k] = jnp.where(mine, first, colacc[1, k])

    def back_first(i):
        at = rows_at(i)
        value = []
        for j in range(blocks):
            e, f = ef[0, at, cut(j)], ef[1, at, cut(j)]
            eo, fo = efo[0, at, cut(j)], efo[1, at, cut(j)]
            v = vm[at, cut(j)]
            shared = 1.0 / (e * eo + v * (e + eo))
            own, cross = (eo + v) * shared, v * shared
            mid[0, at, cut(j)] = own
            mid[1, at, cut(j)] = cross
            value.append(own * f + cross * fo)
        back(zb, i, value)

    def back_second(i):
        at = rows_at(i)
        back(vb, i, [mid[0, at, cut(j)] * f2[at, cut(j)] + mid[1, at, cut(j)] * f2o[at, cut(j)] for j in range(blocks)])

    def send_part(field, trip, part, side_of):
        at = S if side_of else rows + S - 1
        for k in range(depth):
            row_s[trip, side_of, k:k + 1, :] = field[lay[k], at:at + 1, :]
            final = jnp.sum(colacc[0, k], axis=0, keepdims=True)
            col_s[trip, part, 0, k:k + 1, :] = final * col_s[0, 0, 0, k:k + 1, :]
            col_s[trip, part, 1, k:k + 1, :] = jnp.sum(colacc[1, k], axis=0, keepdims=True)
        send_halo(trip, (side_of, 2 + 2 * part, 3 + 2 * part))

    def receive_row(field, trip, side_of):
        at = rows + S if side_of else S - 1
        take_halo(trip, (side_of,))
        for k in range(depth):
            field[lay[k], at:at + 1, :] = row_r[trip, side_of, k:k + 1, :]

    def low_tiles(p):
        return jnp.where(p < tiles - per - 1, p + per, jnp.where(p < tiles - 1, tiles - 2 - p, tiles - 1))

    def high_tiles(p):
        return lax.rem(p + 1, tiles)

    def sideways(field, i, k, outside=None):
        at, pad, ahead = rows_at(i), rows_at(i + 1), rows_at(i + 2)
        value = [field[lay[k], pad, cut(j)] for j in range(blocks)]
        c = [cb[lay[k], at, cut(j)] for j in range(blocks)]
        outside = spread_c[k, at, :] if outside is None else outside
        turned = [(pltpu.roll(c[j] * value[j], 1, 1), pltpu.roll(value[j], L - 1, 1)) for j in range(blocks)]
        to_right = [jnp.where(first_lane, turned[j - 1][0] if j else outside, turned[j][0]) for j in range(blocks)]
        beside = [jnp.where(final_lane, turned[j + 1][1] if j < blocks - 1 else outside, turned[j][1])
                  for j in range(blocks)]
        for j in range(blocks):
            r = rb[lay[k], pad, cut(j)]
            down = r * value[j]
            before = rb[lay[k], at, cut(j)] * field[lay[k], at, cut(j)]
            term = r * next_row(value[j], field[lay[k], ahead, cut(j)]) + prev_row(down, before)
            side[k, :, cut(j)] = term + (c[j] * beside[j] + to_right[j])

    def first_sides(field, trip):
        i = per if trip == 1 else 1
        at, end = pl.ds(i * S, S), cut(blocks - 1)
        for k in range(depth):
            sideways(field, i, k, jnp.zeros((S, L), F32))
        take_halo(trip, (2, 3))
        spread(col_r.at[trip, 0])
        for k in range(depth):
            outside = spread_c[k, at, :]
            side[k, :, cut(0)] += jnp.where(first_lane, outside, 0.0)
            side[k, :, end] += cb[lay[k], at, end] * jnp.where(final_lane, outside, 0.0)

    def take_columns(trip):
        take_halo(trip, (4, 5))
        spread(col_r.at[trip, 1])

    def images(field, trip, order, begin, carry, after=None):
        needs = [(tiles - per - 1, lambda: take_columns(trip)),
                 (tiles - 2 if trip == 1 else tiles - 1, lambda: receive_row(field, trip, 0)),
                 (tiles - 1 if trip == 1 else tiles - 2, lambda: receive_row(field, trip, 1))]

        def chunk(q, carry):
            for j in range(per):
                for place, take in needs:
                    if (place - 1) % per == j:
                        pl.when(q == (place - 1) // per)(take)
                position = q * per + j
                use, ahead = begin(order(position)), order(lax.rem(position + 1, tiles))
                for k in range(depth):
                    carry = use(k, [side[k, :, cut(b)] for b in range(blocks)], carry)
                    sideways(field, ahead, k)
            if after is not None:
                after(q)
            return carry

        return lax.fori_loop(0, chunks, chunk, carry)

    def down(total):
        return jnp.sum(total, axis=0, keepdims=True)

    def across(total):
        return jnp.sum(total, axis=1, keepdims=True)

    def pair_copy(slot):
        return remote(pair_s.at[slot], pair_r.at[slot], pair_sem.at[slot], partner)

    def pair_begin(slot, totals):
        for q, total in enumerate(totals):
            pair_s[slot, q:q + 1, :] = down(total)
        pair_copy(slot).start()

    def pair_finish(slot):
        pair_copy(slot).wait_recv()
        return across(pair_s[slot] + pair_r[slot])

    def sum_copies():
        def way(o, n):
            return min(o, n - o)

        offsets = [(a, b) for a in range(npx) for b in range(npy) if a or b]
        offsets.sort(key=lambda o: -way(o[0] // deep, wide) - way(o[0] % deep, deep) - way(o[1], npy))
        to_x, to_y = [lax.rem(px + a, npx) for a in range(npx)], [lax.rem(py + b, npy) for b in range(npy)]
        return [remote(sum_s, sum_r.at[me], sum_sem, (up, to_x[a], to_y[b])) for a, b in offsets]

    def sum_bytes(end):
        part = sum_r.at[pl.ds(0, peers - 1)]
        return pltpu.make_async_copy(part, part, sum_sem.at[end])

    heard(0)
    colacc[...] = jnp.zeros_like(colacc)

    def wait_middle(c):
        ef_copy(c).wait_recv()
        pl.when(up == 1)(vm_copy(c).wait_recv)

    in_chunks(back_first, before=wait_middle,
              after=lambda c: pl.when(c == chunks - 1)(lambda: send_part(zb, 1, 0, 0)))
    send_part(zb, 1, 1, 1)

    zero = jnp.zeros((S, L), F32)

    def image_first(i):
        at, pad = rows_at(i), rows_at(i + 1)
        y = [None] * blocks

        def use(k, terms, sums):
            one, two = sums
            for j in range(blocks):
                b, value = bb[lay[k], at, cut(j)], zb[lay[k], pad, cut(j)]
                w = b - terms[j]
                wb[lay[k], at, cut(j)] = w
                one = one + b * value
                two = two + w * value
                y[j] = w if k == 0 else w + gain[k - 1, at, cut(j)] * y[j]
                if k < last:
                    vb[lay[k], pad, cut(j)] = y[j] * inv[k, at, cut(j)]
                else:
                    f2[at, cut(j)] = y[j]
            return one, two

        return use

    first_sides(zb, 1)
    heard(1)
    one, two = images(zb, 1, low_tiles, image_first, (zero, zero),
                      after=lambda q: pl.when(q < chunks - 2)(lambda: f2_copy(q + 1).start()))
    f2_copy(0).start()
    f2_copy(chunks - 1).start()
    pair_begin(0, (one, two))
    in_chunks(back_second, order=high_last, before=lambda c: f2_copy(c).wait_recv(),
              after=lambda c: pl.when(c == 0)(lambda: send_part(vb, 2, 0, 1)))
    send_part(vb, 2, 1, 0)
    heard(2)
    here = pair_finish(0)
    rho_here, power_here = here[0:1], here[1:2]
    known = power_here > 0.0
    guess = jnp.where(known, jnp.clip(rho_here / jnp.where(known, power_here, 1.0), 0.25, 256.0), 1.0)
    step = jnp.broadcast_to(guess, (S, L))
    first_sides(vb, 2)

    def image_second(i):
        at, pad = rows_at(i), rows_at(i + 1)

        def use(k, terms, sums):
            rp, wv, qp, uv, uz = sums
            for j in range(blocks):
                w, v, z = wb[lay[k], at, cut(j)], vb[lay[k], pad, cut(j)], zb[lay[k], pad, cut(j)]
                u = w - terms[j]
                ut[lay[k], at, cut(j)] = u
                p = z - step * v
                rp = rp + (bb[lay[k], at, cut(j)] - step * w) * p
                wv = wv + w * v
                qp = qp + (w - step * u) * p
                uv = uv + u * v
                uz = uz + u * z
            return rp, wv, qp, uv, uz

        return use

    sums = images(vb, 2, high_tiles, image_second, (zero,) * 5)
    pair_begin(1, sums)
    for t in range(3, len(rounds)):
        heard(t)
    here = pair_finish(1)
    rp, wv, qp, uv, uz = [here[q:q + 1] for q in range(5)]
    entries = [rp, qp, power_here - guess * wv, 0.5 * (wv + uz) - guess * uv, wv, uv, guess, guess, rho_here, power_here]
    row = jnp.zeros((1, L), F32)
    for q, entry in enumerate(entries):
        row = jnp.where(lane[0:1] == q, entry, row)
    sum_s[...] = row
    sum_r[me] = row

    for copy in sum_copies():
        copy.start()

    end_halo(0, (0, 2))
    end_halo(1, range(6))
    end_halo(2, range(6))
    all_sent(ef, ef_sem)
    all_sent(f2, f2_sem)
    pl.when(lower)(lambda: all_sent(vm, vm_sem))
    pair_copy(0).wait_send()
    pair_copy(1).wait_send()

    def pick(total, q):
        return across(jnp.where(lane[0:1] == q, total, 0.0))

    sum_bytes(1).wait()
    rows_all = sum_r[...].reshape(peers, L)
    total = down(rows_all)
    rho = pick(total, 8)
    alpha = rho / pick(total, 9)
    off = alpha - pltpu.roll(rows_all, L - 6, 1)
    total = down(rows_all - off * (2.0 * pltpu.roll(rows_all, L - 2, 1) - off * pltpu.roll(rows_all, L - 4, 1)))
    rho_next, curvature = pick(total, 0), pick(total, 1)
    ratio = rho_next / rho
    beta = rho_next / (curvature - ratio * rho_next / alpha)
    coef[0] = jnp.broadcast_to(alpha + beta * (1.0 + ratio), (S, L))
    coef[1] = jnp.broadcast_to(beta * alpha, (S, L))

    sum_bytes(0).wait()


def finish(chunks, bb, zb, vb, wb, ut, coef, x_hbm, res_hbm, xb, resb, out_sem):
    depth, rows, width = bb.shape
    chunk_rows = rows // chunks
    on_z, on_v = coef[0], coef[1]

    def out_copies(at):
        return [pltpu.make_async_copy(xb.at[:, at], x_hbm.at[:, at], out_sem.at[0]),
                pltpu.make_async_copy(resb.at[:, at], res_hbm.at[:, at], out_sem.at[1])]

    for c in range(chunks):
        def tile(t, _):
            start = pl.multiple_of(c * chunk_rows + t * S, S)
            at, pad = pl.ds(start, S), pl.ds(pl.multiple_of(start + S, S), S)
            for k in range(depth):
                for j in range(width // L):
                    cut = pl.ds(j * L, L)
                    xb[k, at, cut] = on_z * zb[k, pad, cut] - on_v * vb[k, pad, cut]
                    resb[k, at, cut] = bb[k, at, cut] - on_z * wb[k, at, cut] + on_v * ut[k, at, cut]
            return 0

        lax.fori_loop(0, chunk_rows // S, tile, 0)
        for copy in out_copies(pl.ds(c * chunk_rows, chunk_rows)):
            copy.start()
    for copy in out_copies(pl.ds(0, rows)):
        copy.wait()


def solution(mesh):
    sizes = tuple(mesh.shape[name] for name in ("layer", "px", "py"))
    members, npx, npy = sizes
    assert members == 2

    def shards(*arrays):
        depth, rows, width = arrays[0].shape
        assert rows <= L and rows % S == 0 and width % L == 0 and depth >= 2
        chunks = max(c for c in (2, 4) if (rows // S) % c == 0)
        peers = npx * npy
        full, plane, inner = (depth, rows, width), (rows, width), (depth - 1, rows, width)
        padded = (depth, rows + 2 * S, width)
        dma = pltpu.SemaphoreType.DMA

        def vmem(*shape, dtype=F32):
            return pltpu.VMEM(shape, dtype)

        scratch = [
            vmem(depth, rows + S, width), vmem(*full), vmem(*inner), vmem(*inner, dtype=jnp.int32), vmem(*full),
            vmem(*plane), vmem(*plane, dtype=jnp.int32),
            vmem(*inner), vmem(*inner), vmem(2, *plane), vmem(2, *plane), vmem(2, *plane), vmem(*plane), vmem(*plane),
            vmem(depth, S, width), vmem(depth, rows, L), vmem(depth, rows, L), vmem(depth, S, width), vmem(2, depth, S, L),
            vmem(3, 2, depth, width), vmem(3, 2, depth, width), vmem(3, 2, 2, depth, L), vmem(3, 2, 2, depth, L),
            vmem(2, S, L), vmem(2, S, L), vmem(1, L), vmem(peers, 1, L),
            pltpu.SemaphoreType.REGULAR((4,)),
            dma((chunks,)), dma((2,)), dma((chunks + 1,)), dma((chunks + 1,)), dma((chunks + 1,)), dma((3, 6)),
            dma((2, 2)), dma((2,)),
        ]
        anywhere = pl.BlockSpec(memory_space=pl.ANY)
        kept = pl.pallas_call(
            functools.partial(kernel, sizes, chunks),
            out_shape=(vmem(*full), vmem(*padded), vmem(*padded), vmem(*full), vmem(*full), vmem(2, S, L)),
            in_specs=[anywhere] * 6,
            out_specs=(pl.BlockSpec(memory_space=pltpu.VMEM),) * 6,
            scratch_shapes=scratch,
            compiler_params=pltpu.CompilerParams(
                collective_id=0, has_side_effects=True, vmem_limit_bytes=52 * 1024 * 1024),
            name="pcg",
        )(*arrays)
        return pl.pallas_call(
            functools.partial(finish, 2 * chunks if rows % (2 * chunks * S) == 0 else chunks),
            out_shape=(jax.ShapeDtypeStruct(full, F32), jax.ShapeDtypeStruct(full, F32)),
            in_specs=[pl.BlockSpec(memory_space=pltpu.VMEM)] * 6,
            out_specs=(anywhere,) * 2,
            scratch_shapes=[vmem(*full), vmem(*full), dma((2,))],
            compiler_params=pltpu.CompilerParams(vmem_limit_bytes=8 * 1024 * 1024),
            name="finish",
        )(*kept)

    spec = P("layer", "px", "py")
    return jax.shard_map(shards, mesh=mesh, in_specs=(spec,) * 6, out_specs=(spec, spec), check_vma=False)
```

```python
import functools

import jax
import jax.numpy as jnp
from jax import lax
from jax.experimental import pallas as pl
from jax.experimental.pallas import tpu as pltpu
from jax.sharding import PartitionSpec as P

MESH = pl.DeviceIdType.MESH
S = 8
L = 128
F32 = jnp.float32


def kernel(sizes, chunks, b_hbm, r_hbm, c_hbm, via_hbm, mask_hbm, g_hbm, bb, zb, vb, wb, ut, coef,
           rb, cb, ub, mb, gb, vm, vmask, gain, inv, mid, ef, efo, f2, f2o,
           redge, cedge, spread_c, side, colacc, row_s, row_r, col_s, col_r, pair_s, pair_r, sum_s, sum_r,
           hello_sem, load_sem, edge_sem, vm_sem, ef_sem, f2_sem, halo_sem, pair_sem, sum_sem):
    members, npx, npy = sizes
    depth, rows, width = bb.shape
    tiles = rows // S
    per = tiles // chunks
    last = depth - 1
    blocks = width // L
    up = lax.axis_index("layer")
    px = lax.axis_index("px")
    py = lax.axis_index("py")
    lower = up == 0
    lay = [k + up * (last - 2 * k) for k in range(depth)]
    via_at = [k + up * (last - 1 - 2 * k) for k in range(last)]
    chunk_rows = per * S
    peers = npx * npy
    me = px * npy + py

    partner = (1 - up, px, py)
    above, below = (up, px - 1, py), (up, px + 1, py)
    left, right = (up, px, py - 1), (up, px, py + 1)

    row_r[...] = jnp.zeros_like(row_r)
    pair_s[...] = jnp.zeros_like(pair_s)
    col_r[...] = jnp.zeros_like(col_r)
    barrier = pltpu.get_barrier_semaphore()

    deep = max(d for d in range(1, npx + 1) if npx % d == 0 and d * d <= npx)
    wide = npx // deep
    in_deep = lax.rem(px, deep)
    across_wide = [(up, lax.rem(px + deep * o, npx), py) for o in range(1, wide)]
    along_deep = [(up, px - in_deep + lax.rem(in_deep + o, deep), py) for o in range(1, deep)]
    along_py = [(up, px, lax.rem(py + o, npy)) for o in range(1, npy)]
    mates = [(None, device) for device in across_wide + along_deep + along_py]

    def within(reach):
        found = []
        for o in [o for r in range(1, reach + 1) for o in (-r, r)]:
            if abs(o) < deep:
                found.append((jnp.logical_and(in_deep + o >= 0, in_deep + o < deep), (up, px + o, py)))
            if abs(o) < npy:
                found.append((jnp.logical_and(py + o >= 0, py + o < npy), (up, px, py + o)))
        return found

    crossing = [] if deep == 1 else [
        (jnp.logical_and(in_deep == deep - 1, px < npx - 1), below), (jnp.logical_and(in_deep == 0, px > 0), above)]
    near = [(None, partner)] + [(None, device) for device in across_wide] + within(1) + crossing
    rounds, reach = [], 1
    while reach < max(deep, npy) - 1:
        rounds.append(within(reach))
        reach *= 2
    rounds += [mates, mates]
    assert len(rounds) <= hello_sem.shape[0]

    def greet(sem, targets):
        for exists, device in targets:
            def signal(device=device):
                pl.semaphore_signal(sem, inc=1, device_id=device, device_id_type=MESH)

            signal() if exists is None else pl.when(exists)(signal)

    def count(targets):
        return sum(1 if exists is None else exists.astype(jnp.int32) for exists, _ in targets)

    def hello(t):
        greet(hello_sem.at[t], rounds[t])

    def heard(t):
        if t < len(rounds):
            pl.semaphore_wait(hello_sem.at[t], count(rounds[t]))
        if t + 1 < len(rounds):
            hello(t + 1)

    greet(barrier, near)

    edge_loads = [
        pltpu.make_async_copy(r_hbm.at[:, pl.ds(rows - S, S)], redge, edge_sem.at[0]),
        pltpu.make_async_copy(c_hbm.at[:, :, pl.ds(width - L, L)], cedge, edge_sem.at[1]),
    ]
    for copy in edge_loads:
        copy.start()

    def chunk_at(c, ahead=0):
        start = c * chunk_rows + ahead
        return pl.ds(start if isinstance(start, int) else pl.multiple_of(start, S), chunk_rows)

    def top(c):
        at = chunk_at(c)
        return [pltpu.make_async_copy(via_hbm.at[last, at], vm.at[at], load_sem.at[c]),
                pltpu.make_async_copy(mask_hbm.at[last, at], vmask.at[at], load_sem.at[c])]

    def loads(c):
        at = chunk_at(c)
        inner = pl.ds(0, last)
        pairs = [(c_hbm.at[:, at], cb.at[:, at]),
                 (g_hbm.at[:, at], gb.at[:, at]), (via_hbm.at[inner, at], ub.at[:, at]),
                 (mask_hbm.at[inner, at], mb.at[:, at]), (b_hbm.at[:, at], bb.at[:, at])]
        return [pltpu.make_async_copy(src, dst, load_sem.at[c]) for src, dst in pairs]

    def row_load(c):
        start = c * chunk_rows - (S if c == 1 else 0)
        size = chunk_rows + (S if c == 1 else -S if c == 0 else 0)
        return pltpu.make_async_copy(
            r_hbm.at[:, pl.ds(start, size)], rb.at[:, pl.ds(start + S, size)], load_sem.at[c])

    def start_loads(c):
        row_load(c).start()
        for copy in loads(c):
            copy.start()

        @pl.when(lower)
        def _():
            for copy in top(c):
                copy.start()

    start_loads(1 % chunks)

    lane = lax.broadcasted_iota(jnp.int32, (S, L), 1)
    sub = lax.broadcasted_iota(jnp.int32, (S, L), 0)
    first_lane, final_lane = lane == 0, lane == L - 1
    first_sub, final_sub = sub == 0, sub == S - 1

    def remote(src, dst, sems, device):
        return pltpu.make_async_remote_copy(
            src_ref=src, dst_ref=dst, send_sem=sems.at[0], recv_sem=sems.at[1],
            device_id=device, device_id_type=MESH)

    def exchanges(trip):
        def one(e, src, dst, device):
            return pltpu.make_async_remote_copy(
                src_ref=src, dst_ref=dst, send_sem=halo_sem.at[2, 0], recv_sem=halo_sem.at[trip % 2, e],
                device_id=device, device_id_type=MESH)

        down_up = [
            (px < npx - 1, px > 0, one(0, row_s.at[trip, 0], row_r.at[trip, 0], below)),
            (px > 0, px < npx - 1, one(1, row_s.at[trip, 1], row_r.at[trip, 1], above)),
        ]
        for part in range(2):
            sent, got = col_s.at[trip, part], col_r.at[trip, part]
            down_up.append((py < npy - 1, py > 0, one(2 + 2 * part, sent.at[0], got.at[0], right)))
            down_up.append((py > 0, py < npy - 1, one(3 + 2 * part, sent.at[1], got.at[1], left)))
        return down_up

    def send_halo(trip, which):
        for e in which:
            sends, _, copy = exchanges(trip)[e]
            pl.when(sends)(copy.start)

    def take_halo(trip, which):
        for e in which:
            sends, takes, copy = exchanges(trip)[e]
            pl.when(takes)(copy.wait_recv)

    def end_halo(trip, which):
        for e in which:
            sends, _, copy = exchanges(trip)[e]
            pl.when(sends)(copy.wait_send)

    edge_loads[0].wait()
    for c in range(1, chunks):
        start_loads((1 + c) % chunks)
    for k in range(depth):
        row_s[0, 0, k:k + 1, :] = redge[lay[k], S - 1:S, :]
    edge_loads[1].wait()
    for k in range(depth):
        acc = jnp.zeros((S, L), F32)
        for i in range(tiles):
            edge = jnp.broadcast_to(cedge[lay[k], i * S:(i + 1) * S, L - 1:L], (S, L))
            acc = jnp.where(lane == sub + i * S, edge, acc)
        col_s[0, 0, 0, k:k + 1, :] = jnp.sum(acc, axis=0, keepdims=True)
    pl.semaphore_wait(barrier, count(near))
    send_halo(0, (2, 0))
    hello(0)
    take_halo(0, (2,))

    def spread(ref):
        for k in range(depth):
            both = jnp.concatenate([jnp.broadcast_to(ref[side_of, k:k + 1, :], (L // 2, L)) for side_of in range(2)], axis=0)
            spread_c[k] = jnp.transpose(both)[:rows]

    def rows_at(i):
        return pl.ds(pl.multiple_of(i * S, S), S)

    def cut(j):
        return pl.ds(j * L, L)

    def next_row(now, after):
        return pltpu.roll(jnp.where(first_sub, after, now), S - 1, 0)

    def prev_row(now, before):
        return pltpu.roll(jnp.where(final_sub, before, now), 1, 0)

    def from_left(parts, edge):
        turned = [pltpu.roll(p, 1, 1) for p in parts]
        return [jnp.where(first_lane, turned[j - 1] if j else edge, turned[j]) for j in range(blocks)]

    def factor_tile(i):
        at, pad = rows_at(i), rows_at(i + 1)
        coupling, g, y = [None] * blocks, [None] * blocks, [None] * blocks
        for k in range(depth):
            edge = spread_c[k, at, :]
            c = [cb[lay[k], at, cut(j)] for j in range(blocks)]
            c_left = from_left(c, edge)
            for j in range(blocks):
                r = rb[lay[k], pad, cut(j)]
                d = gb[lay[k], at, cut(j)] + r + prev_row(r, rb[lay[k], at, cut(j)]) + c[j] + c_left[j]
                rhs = bb[lay[k], at, cut(j)]
                if k:
                    d = d + coupling[j] - coupling[j] * g[j]
                    rhs = rhs + g[j] * y[j]
                y[j] = rhs
                if k < last:
                    coupling[j] = ub[via_at[k], at, cut(j)] * mb[via_at[k], at, cut(j)].astype(F32)
                    inverse = 1.0 / (d + coupling[j])
                    g[j] = coupling[j] * inverse
                    gain[k, at, cut(j)] = g[j]
                    inv[k, at, cut(j)] = inverse
                    zb[lay[k], pad, cut(j)] = rhs * inverse
                else:
                    ef[0, at, cut(j)] = d
                    ef[1, at, cut(j)] = rhs

    def to_partner(src, dst, sems, c):
        return pltpu.make_async_remote_copy(
            src_ref=src, dst_ref=dst, send_sem=sems.at[chunks], recv_sem=sems.at[c],
            device_id=partner, device_id_type=MESH)

    def all_sent(ref, sems):
        pltpu.make_async_copy(ref, ref, sems.at[chunks]).wait()

    def vm_copy(c):
        return to_partner(vm.at[chunk_at(c)], vm.at[chunk_at(c)], vm_sem, c)

    def ef_copy(c):
        return to_partner(ef.at[:, chunk_at(c)], efo.at[:, chunk_at(c)], ef_sem, c)

    def f2_copy(c):
        return to_partner(f2.at[chunk_at(c)], f2o.at[chunk_at(c)], f2_sem, c)

    def low_last(q):
        return lax.rem(q + 1, chunks)

    def high_last(q):
        return jnp.where(q < chunks - 2, q + 1, jnp.where(q == chunks - 2, 0, chunks - 1))

    def in_chunks(tile, order=low_last, before=None, after=None):
        def chunk(q, _):
            c = order(q)
            if before is not None:
                before(c)

            def one(j, _):
                tile(c * per + j)
                return 0

            lax.fori_loop(0, per, one, 0)
            if after is not None:
                after(c)
            return 0

        lax.fori_loop(0, chunks, chunk, 0)

    def wait_loads(c):
        for one in range(chunks):
            pl.when(c == one)(row_load(one).wait)
        for copy in loads(c):
            copy.wait()

        @pl.when(c == 0)
        def _():
            take_halo(0, (0,))
            for k in range(depth):
                rb[lay[k], S - 1:S, :] = row_r[0, 0, k:k + 1, :]

        @pl.when(lower)
        def _():
            for copy in top(c):
                copy.wait()

        @pl.when(lower)
        def _():
            def times(j, _):
                at = rows_at(c * per + j)
                for b in range(blocks):
                    vm[at, cut(b)] = vm[at, cut(b)] * vmask[at, cut(b)].astype(F32)
                return 0

            lax.fori_loop(0, per, times, 0)
            vm_copy(c).start()

    spread(col_r.at[0, 0])
    in_chunks(factor_tile, before=wait_loads, after=lambda c: ef_copy(c).start())

    def back(field, i, own):
        at, pad = rows_at(i), rows_at(i + 1)
        mine = lane == sub + i * S
        value = own
        for k in range(last, -1, -1):
            for j in range(blocks):
                if k < last:
                    value[j] = field[lay[k], pad, cut(j)] + gain[k, at, cut(j)] * value[j]
                field[lay[k], pad, cut(j)] = value[j]
            first = jnp.broadcast_to(value[0][:, 0:1], (S, L))
            final = jnp.broadcast_to(value[blocks - 1][:, L - 1:L], (S, L))
            colacc[0, k] = jnp.where(mine, final, colacc[0, k])
            colacc[1, k] = jnp.where(mine, first, colacc[1, k])

    def back_first(i):
        at = rows_at(i)
        value = []
        for j in range(blocks):
            e, f = ef[0, at, cut(j)], ef[1, at, cut(j)]
            eo, fo = efo[0, at, cut(j)], efo[1, at, cut(j)]
            v = vm[at, cut(j)]
            shared = 1.0 / (e * eo + v * (e + eo))
            own, cross = (eo + v) * shared, v * shared
            mid[0, at, cut(j)] = own
            mid[1, at, cut(j)] = cross
            value.append(own * f + cross * fo)
        back(zb, i, value)

    def back_second(i):
        at = rows_at(i)
        back(vb, i, [mid[0, at, cut(j)] * f2[at, cut(j)] + mid[1, at, cut(j)] * f2o[at, cut(j)] for j in range(blocks)])

    def send_part(field, trip, part, side_of):
        at = S if side_of else rows + S - 1
        for k in range(depth):
            row_s[trip, side_of, k:k + 1, :] = field[lay[k], at:at + 1, :]
            final = jnp.sum(colacc[0, k], axis=0, keepdims=True)
            col_s[trip, part, 0, k:k + 1, :] = final * col_s[0, 0, 0, k:k + 1, :]
            col_s[trip, part, 1, k:k + 1, :] = jnp.sum(colacc[1, k], axis=0, keepdims=True)
        send_halo(trip, (side_of, 2 + 2 * part, 3 + 2 * part))

    def receive_row(field, trip, side_of):
        at = rows + S if side_of else S - 1
        take_halo(trip, (side_of,))
        for k in range(depth):
            field[lay[k], at:at + 1, :] = row_r[trip, side_of, k:k + 1, :]

    def low_tiles(p):
        return jnp.where(p < tiles - per - 1, p + per, jnp.where(p < tiles - 1, tiles - 2 - p, tiles - 1))

    def high_tiles(p):
        return lax.rem(p + 1, tiles)

    def sideways(field, i, k, outside=None):
        at, pad, ahead = rows_at(i), rows_at(i + 1), rows_at(i + 2)
        value = [field[lay[k], pad, cut(j)] for j in range(blocks)]
        c = [cb[lay[k], at, cut(j)] for j in range(blocks)]
        outside = spread_c[k, at, :] if outside is None else outside
        turned = [(pltpu.roll(c[j] * value[j], 1, 1), pltpu.roll(value[j], L - 1, 1)) for j in range(blocks)]
        to_right = [jnp.where(first_lane, turned[j - 1][0] if j else outside, turned[j][0]) for j in range(blocks)]
        beside = [jnp.where(final_lane, turned[j + 1][1] if j < blocks - 1 else outside, turned[j][1])
                  for j in range(blocks)]
        for j in range(blocks):
            r = rb[lay[k], pad, cut(j)]
            down = r * value[j]
            before = rb[lay[k], at, cut(j)] * field[lay[k], at, cut(j)]
            term = r * next_row(value[j], field[lay[k], ahead, cut(j)]) + prev_row(down, before)
            side[k, :, cut(j)] = term + (c[j] * beside[j] + to_right[j])

    def first_sides(field, trip):
        i = per if trip == 1 else 1
        at, end = pl.ds(i * S, S), cut(blocks - 1)
        for k in range(depth):
            sideways(field, i, k, jnp.zeros((S, L), F32))
        take_halo(trip, (2, 3))
        spread(col_r.at[trip, 0])
        for k in range(depth):
            outside = spread_c[k, at, :]
            side[k, :, cut(0)] += jnp.where(first_lane, outside, 0.0)
            side[k, :, end] += cb[lay[k], at, end] * jnp.where(final_lane, outside, 0.0)

    def take_columns(trip):
        take_halo(trip, (4, 5))
        spread(col_r.at[trip, 1])

    def images(field, trip, order, begin, carry, after=None):
        needs = [(tiles - per - 1, lambda: take_columns(trip)),
                 (tiles - 2 if trip == 1 else tiles - 1, lambda: receive_row(field, trip, 0)),
                 (tiles - 1 if trip == 1 else tiles - 2, lambda: receive_row(field, trip, 1))]

        def chunk(q, carry):
            for j in range(per):
                for place, take in needs:
                    if (place - 1) % per == j:
                        pl.when(q == (place - 1) // per)(take)
                position = q * per + j
                use, ahead = begin(order(position)), order(lax.rem(position + 1, tiles))
                for k in range(depth):
                    carry = use(k, [side[k, :, cut(b)] for b in range(blocks)], carry)
                    sideways(field, ahead, k)
            if after is not None:
                after(q)
            return carry

        return lax.fori_loop(0, chunks, chunk, carry)

    def down(total):
        return jnp.sum(total, axis=0, keepdims=True)

    def across(total):
        return jnp.sum(total, axis=1, keepdims=True)

    def pair_copy(slot):
        return remote(pair_s.at[slot], pair_r.at[slot], pair_sem.at[slot], partner)

    def pair_begin(slot, totals):
        for q, total in enumerate(totals):
            pair_s[slot, q:q + 1, :] = down(total)
        pair_copy(slot).start()

    def pair_finish(slot):
        pair_copy(slot).wait_recv()
        return across(pair_s[slot] + pair_r[slot])

    def sum_copies():
        def way(o, n):
            return min(o, n - o)

        offsets = [(a, b) for a in range(npx) for b in range(npy) if a or b]
        offsets.sort(key=lambda o: -way(o[0] // deep, wide) - way(o[0] % deep, deep) - way(o[1], npy))
        to_x, to_y = [lax.rem(px + a, npx) for a in range(npx)], [lax.rem(py + b, npy) for b in range(npy)]
        return [remote(sum_s, sum_r.at[me], sum_sem, (up, to_x[a], to_y[b])) for a, b in offsets]

    def sum_bytes(end):
        part = sum_r.at[pl.ds(0, peers - 1)]
        return pltpu.make_async_copy(part, part, sum_sem.at[end])

    colacc[...] = jnp.zeros_like(colacc)

    def wait_middle(c):
        ef_copy(c).wait_recv()
        pl.when(up == 1)(vm_copy(c).wait_recv)

    in_chunks(back_first, before=wait_middle,
              after=lambda c: pl.when(c == chunks - 1)(lambda: send_part(zb, 1, 0, 0)))
    send_part(zb, 1, 1, 1)
    heard(0)

    zero = jnp.zeros((S, L), F32)

    def image_first(i):
        at, pad = rows_at(i), rows_at(i + 1)
        y = [None] * blocks

        def use(k, terms, sums):
            one, two = sums
            for j in range(blocks):
                b, value = bb[lay[k], at, cut(j)], zb[lay[k], pad, cut(j)]
                w = b - terms[j]
                wb[lay[k], at, cut(j)] = w
                one = one + b * value
                two = two + w * value
                y[j] = w if k == 0 else w + gain[k - 1, at, cut(j)] * y[j]
                if k < last:
                    vb[lay[k], pad, cut(j)] = y[j] * inv[k, at, cut(j)]
                else:
                    f2[at, cut(j)] = y[j]
            return one, two

        return use

    first_sides(zb, 1)
    one, two = images(zb, 1, low_tiles, image_first, (zero, zero),
                      after=lambda q: pl.when(q < chunks - 2)(lambda: f2_copy(q + 1).start()))
    f2_copy(0).start()
    f2_copy(chunks - 1).start()
    pair_begin(0, (one, two))
    in_chunks(back_second, order=high_last, before=lambda c: f2_copy(c).wait_recv(),
              after=lambda c: pl.when(c == 0)(lambda: send_part(vb, 2, 0, 1)))
    send_part(vb, 2, 1, 0)
    heard(1)
    here = pair_finish(0)
    rho_here, power_here = here[0:1], here[1:2]
    known = power_here > 0.0
    guess = jnp.where(known, jnp.clip(rho_here / jnp.where(known, power_here, 1.0), 0.25, 256.0), 1.0)
    step = jnp.broadcast_to(guess, (S, L))
    first_sides(vb, 2)
    heard(2)

    def image_second(i):
        at, pad = rows_at(i), rows_at(i + 1)

        def use(k, terms, sums):
            rp, wv, qp, uv, uz = sums
            for j in range(blocks):
                w, v, z = wb[lay[k], at, cut(j)], vb[lay[k], pad, cut(j)], zb[lay[k], pad, cut(j)]
                u = w - terms[j]
                ut[lay[k], at, cut(j)] = u
                p = z - step * v
                rp = rp + (bb[lay[k], at, cut(j)] - step * w) * p
                wv = wv + w * v
                qp = qp + (w - step * u) * p
                uv = uv + u * v
                uz = uz + u * z
            return rp, wv, qp, uv, uz

        return use

    sums = images(vb, 2, high_tiles, image_second, (zero,) * 5)
    pair_begin(1, sums)
    for t in range(3, len(rounds)):
        heard(t)
    here = pair_finish(1)
    rp, wv, qp, uv, uz = [here[q:q + 1] for q in range(5)]
    entries = [rp, qp, power_here - guess * wv, 0.5 * (wv + uz) - guess * uv, wv, uv, guess, guess, rho_here, power_here]
    row = jnp.zeros((1, L), F32)
    for q, entry in enumerate(entries):
        row = jnp.where(lane[0:1] == q, entry, row)
    sum_s[...] = row
    sum_r[me] = row

    for copy in sum_copies():
        copy.start()

    end_halo(0, (0, 2))
    end_halo(1, range(6))
    end_halo(2, range(6))
    all_sent(ef, ef_sem)
    all_sent(f2, f2_sem)
    pl.when(lower)(lambda: all_sent(vm, vm_sem))
    pair_copy(0).wait_send()
    pair_copy(1).wait_send()

    def pick(total, q):
        return across(jnp.where(lane[0:1] == q, total, 0.0))

    sum_bytes(1).wait()
    rows_all = sum_r[...].reshape(peers, L)
    total = down(rows_all)
    rho = pick(total, 8)
    alpha = rho / pick(total, 9)
    off = alpha - pltpu.roll(rows_all, L - 6, 1)
    total = down(rows_all - off * (2.0 * pltpu.roll(rows_all, L - 2, 1) - off * pltpu.roll(rows_all, L - 4, 1)))
    rho_next, curvature = pick(total, 0), pick(total, 1)
    ratio = rho_next / rho
    beta = rho_next / (curvature - ratio * rho_next / alpha)
    coef[0] = jnp.broadcast_to(alpha + beta * (1.0 + ratio), (S, L))
    coef[1] = jnp.broadcast_to(beta * alpha, (S, L))

    sum_bytes(0).wait()


def finish(chunks, bb, zb, vb, wb, ut, coef, x_hbm, res_hbm, xb, resb, out_sem):
    depth, rows, width = bb.shape
    chunk_rows = rows // chunks
    on_z, on_v = coef[0], coef[1]

    def out_copies(at):
        return [pltpu.make_async_copy(xb.at[:, at], x_hbm.at[:, at], out_sem.at[0]),
                pltpu.make_async_copy(resb.at[:, at], res_hbm.at[:, at], out_sem.at[1])]

    for c in range(chunks):
        def tile(t, _):
            start = pl.multiple_of(c * chunk_rows + t * S, S)
            at, pad = pl.ds(start, S), pl.ds(pl.multiple_of(start + S, S), S)
            for k in range(depth):
                for j in range(width // L):
                    cut = pl.ds(j * L, L)
                    xb[k, at, cut] = on_z * zb[k, pad, cut] - on_v * vb[k, pad, cut]
                    resb[k, at, cut] = bb[k, at, cut] - on_z * wb[k, at, cut] + on_v * ut[k, at, cut]
            return 0

        lax.fori_loop(0, chunk_rows // S, tile, 0)
        for copy in out_copies(pl.ds(c * chunk_rows, chunk_rows)):
            copy.start()
    for copy in out_copies(pl.ds(0, rows)):
        copy.wait()


def solution(mesh):
    sizes = tuple(mesh.shape[name] for name in ("layer", "px", "py"))
    members, npx, npy = sizes
    assert members == 2

    def shards(*arrays):
        depth, rows, width = arrays[0].shape
        assert rows <= L and rows % S == 0 and width % L == 0 and depth >= 2
        chunks = max(c for c in (2, 4) if (rows // S) % c == 0)
        peers = npx * npy
        full, plane, inner = (depth, rows, width), (rows, width), (depth - 1, rows, width)
        padded = (depth, rows + 2 * S, width)
        dma = pltpu.SemaphoreType.DMA

        def vmem(*shape, dtype=F32):
            return pltpu.VMEM(shape, dtype)

        scratch = [
            vmem(depth, rows + S, width), vmem(*full), vmem(*inner), vmem(*inner, dtype=jnp.int32), vmem(*full),
            vmem(*plane), vmem(*plane, dtype=jnp.int32),
            vmem(*inner), vmem(*inner), vmem(2, *plane), vmem(2, *plane), vmem(2, *plane), vmem(*plane), vmem(*plane),
            vmem(depth, S, width), vmem(depth, rows, L), vmem(depth, rows, L), vmem(depth, S, width), vmem(2, depth, S, L),
            vmem(3, 2, depth, width), vmem(3, 2, depth, width), vmem(3, 2, 2, depth, L), vmem(3, 2, 2, depth, L),
            vmem(2, S, L), vmem(2, S, L), vmem(1, L), vmem(peers, 1, L),
            pltpu.SemaphoreType.REGULAR((4,)),
            dma((chunks,)), dma((2,)), dma((chunks + 1,)), dma((chunks + 1,)), dma((chunks + 1,)), dma((3, 6)),
            dma((2, 2)), dma((2,)),
        ]
        anywhere = pl.BlockSpec(memory_space=pl.ANY)
        kept = pl.pallas_call(
            functools.partial(kernel, sizes, chunks),
            out_shape=(vmem(*full), vmem(*padded), vmem(*padded), vmem(*full), vmem(*full), vmem(2, S, L)),
            in_specs=[anywhere] * 6,
            out_specs=(pl.BlockSpec(memory_space=pltpu.VMEM),) * 6,
            scratch_shapes=scratch,
            compiler_params=pltpu.CompilerParams(
                collective_id=0, has_side_effects=True, vmem_limit_bytes=52 * 1024 * 1024),
            name="pcg",
        )(*arrays)
        return pl.pallas_call(
            functools.partial(finish, 2 * chunks if rows % (2 * chunks * S) == 0 else chunks),
            out_shape=(jax.ShapeDtypeStruct(full, F32), jax.ShapeDtypeStruct(full, F32)),
            in_specs=[pl.BlockSpec(memory_space=pltpu.VMEM)] * 6,
            out_specs=(anywhere,) * 2,
            scratch_shapes=[vmem(*full), vmem(*full), dma((2,))],
            compiler_params=pltpu.CompilerParams(vmem_limit_bytes=8 * 1024 * 1024),
            name="finish",
        )(*kept)

    spec = P("layer", "px", "py")
    return jax.shard_map(shards, mesh=mesh, in_specs=(spec,) * 6, out_specs=(spec, spec), check_vma=False)
```
